8 devices in a mesh: dp: 2 (over z, y), x: 4 (over x, core).
Axes of the slice: x: 2, y: 2, z: 1, core: 2. Of those that a mesh axis runs over, the one named last changes fastest.
Arguments:
- start_pos: int32 [256], P('dp'), parts along dimension 0
- hidden_in: bfloat16 [4, 256, 5120], P(None, ('dp', 'x')), parts along dimension 1
- k_cache: bfloat16 [256, 256, 8, 128], P('dp', None, 'x'), parts along dimension 0
- v_cache: bfloat16 [256, 256, 8, 128], P('dp', None, 'x'), parts along dimension 0
- attn_norm: bfloat16 [5120], replicated
- w_q: bfloat16 [5120, 8192], replicated
- w_k: bfloat16 [5120, 1024], replicated
- w_v: bfloat16 [5120, 1024], replicated
- q_norm: bfloat16 [128], replicated
- k_norm: bfloat16 [128], replicated
- w_o: bfloat16 [8192, 5120], replicated
- mlp_norm: bfloat16 [5120], replicated
- w_gate: bfloat16 [5120, 25600], replicated
- w_up: bfloat16 [5120, 25600], replicated
- w_down: bfloat16 [25600, 5120], replicated
Outputs:
- output 1: bfloat16 [4, 256, 5120], P(None, ('dp', 'x')), parts along dimension 1
- output 2: bfloat16 [256, 256, 8, 128], P(('dp', 'x')), parts along dimension 0
- output 3: bfloat16 [256, 256, 8, 128], P(('dp', 'x')), parts along dimension 0
There are 2 independent parts. The reference program is written for one: setup_inputs(seed, part) draws one part's arguments, and reference() takes and returns one part's arrays. A program takes and returns all parts, laid end to end along the dimension named above; an argument that names none is the same for every part.
All inputs are finite; a program needn't handle non-finite values.
Results may differ from the reference program's by a relative error of at most 0.0104383.
Values are sent between devices in bfloat16 or wider.
A program may use at most 4 GiB of HBM per device.

```python
import math
import jax
import jax.numpy as jnp
from jax import lax

BATCH = 128
T = 256
D = 5120
HEADS = 64
KV_HEADS = 8
HEAD = 128
FF = 25600
STEPS = 4

EPS = 1e-6
THETA = 1000000.0
Q_GAIN = math.sqrt(0.8 * math.log(T))
K_GAIN = math.sqrt(2.0 * math.log(T))


def rms_norm(values, gain_vec):
    values32 = values.astype(jnp.float32)
    inv_rms = lax.rsqrt(jnp.mean(values32 * values32, axis=-1, keepdims=True) + EPS)
    return values32 * inv_rms * gain_vec.astype(jnp.float32)


def rotary(values, positions):
    half_dim = HEAD // 2
    inv_freq = jnp.power(THETA, -jnp.arange(half_dim, dtype=jnp.float32) * 2.0 / HEAD)
    angles = positions.astype(jnp.float32)[..., None, None] * inv_freq
    cos_part = jnp.cos(angles)
    sin_part = jnp.sin(angles)
    first_half = values[..., :half_dim]
    second_half = values[..., half_dim:]
    return jnp.concatenate([first_half * cos_part - second_half * sin_part, second_half * cos_part + first_half * sin_part], axis=-1)


def setup_inputs(seed: int = 0, part: int = 0) -> dict:
    base_keys = jax.random.split(jax.random.key(seed), 16)

    def part_normal(index, shape):
        return jax.random.normal(jax.random.fold_in(base_keys[index], part), shape, jnp.float32)

    def shared_normal(index, shape):
        return jax.random.normal(base_keys[index], shape, jnp.float32)

    pos_key = jax.random.fold_in(base_keys[0], part)
    pos_draw = jax.random.randint(jax.random.fold_in(pos_key, 1), (BATCH,), T // 4, T - 3)
    top_row = jax.random.randint(jax.random.fold_in(pos_key, 2), (), 0, BATCH)
    start_pos = jnp.where(jnp.arange(BATCH) == top_row, T - 4, pos_draw).astype(jnp.int32)
    return dict(
        start_pos=start_pos,
        hidden_in=part_normal(1, (STEPS, BATCH, D)).astype(jnp.bfloat16),
        k_cache=part_normal(2, (BATCH, T, KV_HEADS, HEAD)).astype(jnp.bfloat16),
        v_cache=part_normal(3, (BATCH, T, KV_HEADS, HEAD)).astype(jnp.bfloat16),
        attn_norm=(1.0 + 0.2 * shared_normal(4, (D,))).astype(jnp.bfloat16),
        w_q=(shared_normal(5, (D, HEADS * HEAD)) * D ** -0.5).astype(jnp.bfloat16),
        w_k=(shared_normal(6, (D, KV_HEADS * HEAD)) * D ** -0.5).astype(jnp.bfloat16),
        w_v=(shared_normal(7, (D, KV_HEADS * HEAD)) * D ** -0.5).astype(jnp.bfloat16),
        q_norm=(Q_GAIN * (1.0 + 0.2 * shared_normal(8, (HEAD,)))).astype(jnp.bfloat16),
        k_norm=(K_GAIN * (1.0 + 0.2 * shared_normal(9, (HEAD,)))).astype(jnp.bfloat16),
        w_o=(shared_normal(10, (HEADS * HEAD, D)) * (HEADS * HEAD) ** -0.5).astype(jnp.bfloat16),
        mlp_norm=(1.0 + 0.2 * shared_normal(11, (D,))).astype(jnp.bfloat16),
        w_gate=(shared_normal(12, (D, FF)) * D ** -0.5).astype(jnp.bfloat16),
        w_up=(shared_normal(13, (D, FF)) * D ** -0.5).astype(jnp.bfloat16),
        w_down=(shared_normal(14, (FF, D)) * FF ** -0.5).astype(jnp.bfloat16),
    )


def reference(start_pos, hidden_in, k_cache, v_cache, attn_norm, w_q, w_k, w_v, q_norm, k_norm, w_o, mlp_norm, w_gate, w_up, w_down):
    group_size = HEADS // KV_HEADS
    score_scale = HEAD ** -0.5
    tokens = rms_norm(hidden_in, attn_norm).astype(jnp.bfloat16).reshape(STEPS * BATCH, D)
    queries = jnp.dot(tokens, w_q, preferred_element_type=jnp.float32).reshape(STEPS, BATCH, HEADS, HEAD)
    keys_new = jnp.dot(tokens, w_k, preferred_element_type=jnp.float32).reshape(STEPS, BATCH, KV_HEADS, HEAD)
    values_new = jnp.dot(tokens, w_v, preferred_element_type=jnp.float32).reshape(STEPS, BATCH, KV_HEADS, HEAD)
    positions = start_pos[None, :] + jnp.arange(STEPS)[:, None]
    queries = rotary(rms_norm(queries, q_norm), positions).astype(jnp.bfloat16)
    keys_new = rotary(rms_norm(keys_new, k_norm), positions).astype(jnp.bfloat16)
    values_new = values_new.astype(jnp.bfloat16)

    def one_row(row_inputs):
        row_q, row_k, row_v, row_kc, row_vc, row_pos = row_inputs

        def one_step(carry_in, step_inputs):
            cache_k, cache_v = carry_in
            step_q, step_k, step_v, slot_idx = step_inputs
            cache_k = lax.dynamic_update_slice(cache_k, step_k[None], (slot_idx, 0, 0))
            cache_v = lax.dynamic_update_slice(cache_v, step_v[None], (slot_idx, 0, 0))
            grouped = step_q.reshape(KV_HEADS, group_size, HEAD).astype(jnp.float32)
            scores = jnp.einsum('kgd,tkd->kgt', grouped, cache_k.astype(jnp.float32)) * score_scale
            slot_valid = jnp.arange(T) <= slot_idx
            scores = jnp.where(slot_valid, scores, -jnp.inf)
            weights = jnp.exp(scores - jnp.max(scores, axis=-1, keepdims=True))
            weight_sum = jnp.sum(weights, axis=-1)
            mixed_vals = jnp.einsum('kgt,tkd->kgd', weights.astype(jnp.bfloat16).astype(jnp.float32), cache_v.astype(jnp.float32))
            attended = (mixed_vals / weight_sum[..., None]).astype(jnp.bfloat16).reshape(HEADS * HEAD)
            return (cache_k, cache_v), attended

        (final_k, final_v), step_outs = lax.scan(one_step, (row_kc, row_vc), (row_q, row_k, row_v, row_pos + jnp.arange(STEPS)))
        return step_outs, final_k, final_v

    row_outs, k_out, v_out = lax.map(one_row, (jnp.swapaxes(queries, 0, 1), jnp.swapaxes(keys_new, 0, 1), jnp.swapaxes(values_new, 0, 1), k_cache, v_cache, start_pos))
    attended = jnp.swapaxes(row_outs, 0, 1).reshape(STEPS * BATCH, HEADS * HEAD)
    attn_out = jnp.dot(attended, w_o, preferred_element_type=jnp.float32).reshape(STEPS, BATCH, D)
    residual = (hidden_in.astype(jnp.float32) + attn_out).astype(jnp.bfloat16)
    normed = rms_norm(residual, mlp_norm).astype(jnp.bfloat16).reshape(STEPS * BATCH, D)
    gate_val = jnp.dot(normed, w_gate, preferred_element_type=jnp.float32)
    up_val = jnp.dot(normed, w_up, preferred_element_type=jnp.float32)
    activated = (jax.nn.silu(gate_val) * up_val).astype(jnp.bfloat16)
    down_val = jnp.dot(activated, w_down, preferred_element_type=jnp.float32).reshape(STEPS, BATCH, D)
    out_hidden = (residual.astype(jnp.float32) + down_val).astype(jnp.bfloat16)
    return (out_hidden, k_out, v_out)
```

```python
import jax
import jax.numpy as jnp
from jax import lax
from jax.experimental import pallas as pl
from jax.experimental.pallas import tpu as pltpu
from jax.sharding import PartitionSpec as P

EPS = 1e-6
THETA = 1000000.0
F32 = jnp.float32
BF16 = jnp.bfloat16
MESH = pl.DeviceIdType.MESH

STEPS = 4
ROWS = 32
TOK = STEPS * ROWS
GROUP = 128
D = 5120
HD = 128
QH = 16
FF = 25600
T = 256


def rms_norm(values, gain_vec):
    values32 = values.astype(F32)
    inv_rms = lax.rsqrt(jnp.mean(values32 * values32, axis=-1, keepdims=True) + EPS)
    return values32 * inv_rms * gain_vec.astype(F32)


def partners(me):
    c1 = me + 1 - 2 * lax.rem(me, 2)
    c2 = lax.rem(me + 2, 4)
    c3 = 3 - me
    return c1, c2, c3


def greet(devices):
    barrier = pltpu.get_barrier_semaphore()
    for dev in devices:
        pl.semaphore_signal(barrier, inc=1, device_id={"x": dev}, device_id_type=MESH)
    pl.semaphore_wait(barrier, len(devices))


def remote(src, dst, ssem, rsem, dev):
    return pltpu.make_async_remote_copy(
        src_ref=src, dst_ref=dst, send_sem=ssem, recv_sem=rsem,
        device_id={"x": dev}, device_id_type=MESH)


def qkv_kernel(hn, cos, sin, qg, kg, wq, wk, wv, q_out, kn_out, vn_out,
               hall, ws, qscr, kscr, vscr, wsem, s1, r1, s2, r2, sf, rf):
    me = lax.axis_index("x")
    c1, c2, c3 = partners(me)

    wcopies = []
    for c in range(10):
        if c < 8:
            src = wq.at[:, pl.ds(pl.multiple_of(me * 2048 + c * 256, 256), 256)]
        else:
            src = (wk if c == 8 else wv).at[:, pl.ds(pl.multiple_of(me * 256, 256), 256)]
        wcopies.append(pltpu.make_async_copy(src, ws.at[c], wsem.at[c]))

    greet((c1, c2))
    cross = []
    for s in range(STEPS):
        row = 256 + (s // 2) * 128 + (s % 2) * 32
        cp = remote(hn.at[pl.ds(s * 32, 32)], hall.at[pl.ds(row, 32)], s2.at[s], r2.at[s], c2)
        cp.start()
        cross.append(cp)
    near = remote(hn, hall.at[pl.ds(128, 128)], s1, r1, c1)
    near.start()
    for cp in wcopies:
        cp.start()
    hall[pl.ds(0, 128), :] = hn[...]

    fwd = []
    for s in range(STEPS):
        row = 256 + (s // 2) * 128 + (s % 2) * 32
        fwd.append(remote(hall.at[pl.ds(row, 32)], hall.at[pl.ds(row + 64, 32)], sf.at[s], rf.at[s], c1))

    def table(ref, groups):
        return jnp.concatenate([ref[j * STEPS + s] for j, s in groups], axis=0)

    for blk in range(4):
        if blk == 0:
            groups = [(me, s) for s in range(4)]
        elif blk == 1:
            near.wait_recv()
            groups = [(c1, s) for s in range(4)]
        else:
            lo = (blk - 2) * 2
            for s in (lo, lo + 1):
                cross[s].wait_recv()
                fwd[s].start()
            for s in (lo, lo + 1):
                fwd[s].wait_recv()
            groups = [(c2, lo), (c2, lo + 1), (c3, lo), (c3, lo + 1)]
        cos_b = table(cos, groups)
        sin_b = table(sin, groups)

        def head(val, gain, cos_b=cos_b, sin_b=sin_b):
            inv = lax.rsqrt(jnp.mean(val * val, axis=-1, keepdims=True) + EPS)
            val = val * inv * gain
            return val * cos_b + pltpu.roll(val, 64, 1) * sin_b

        def project(c, blk=blk):
            return jnp.dot(hall[pl.ds(blk * 128, 128), :], ws[c], preferred_element_type=F32)

        def q_chunk(c, carry, blk=blk, head=head, project=project):
            acc = project(c)
            for hh in range(2):
                qscr[pl.ds(2 * c + hh, 128, stride=QH), :] = head(acc[:, hh * HD:(hh + 1) * HD], qg[...])
            return carry

        if blk == 0:
            for c in range(8):
                wcopies[c].wait()
        lax.fori_loop(0, 8, q_chunk, 0)
        if blk == 0:
            wcopies[8].wait()
            wcopies[9].wait()
        k_acc = project(8)
        v_acc = project(9)
        for hh in range(2):
            k_head = head(k_acc[:, hh * HD:(hh + 1) * HD], kg[...])
            v_head = v_acc[:, hh * HD:(hh + 1) * HD]
            for g, (j, s) in enumerate(groups):
                at = pl.ds(j * 256 + s * 2 + hh, 32, stride=8)
                kscr[at, :] = k_head[g * 32:(g + 1) * 32]
                vscr[at, :] = v_head[g * 32:(g + 1) * 32]
        for g, (j, s) in enumerate(groups):
            q_out[s, pl.ds(j * 32, 32)] = qscr[pl.ds(g * 512, 512), :].reshape(32, QH, HD).astype(BF16)
    kn_out[...] = kscr[...].reshape(GROUP, 8, HD).astype(BF16)
    vn_out[...] = vscr[...].reshape(GROUP, 8, HD).astype(BF16)
    for s in range(STEPS):
        cross[s].wait_send()
        fwd[s].wait_send()
    near.wait_send()


def qkv(hn, cos, sin, qg, kg, wq, wk, wv):
    vmem = pl.BlockSpec(memory_space=pltpu.VMEM)
    hbm = pl.BlockSpec(memory_space=pl.ANY)
    dma = pltpu.SemaphoreType.DMA
    return pl.pallas_call(
        qkv_kernel,
        out_shape=(jax.ShapeDtypeStruct((STEPS, GROUP, QH, HD), BF16),
                   jax.ShapeDtypeStruct((GROUP, 8, HD), BF16),
                   jax.ShapeDtypeStruct((GROUP, 8, HD), BF16)),
        in_specs=[vmem] * 5 + [hbm] * 3,
        out_specs=(vmem,) * 3,
        scratch_shapes=[
            pltpu.VMEM((512, D), BF16), pltpu.VMEM((10, D, 256), BF16),
            pltpu.VMEM((128 * QH, HD), F32), pltpu.VMEM((GROUP * 8, HD), F32), pltpu.VMEM((GROUP * 8, HD), F32),
            dma((10,)), dma, dma, dma((4,)), dma((4,)), dma((4,)), dma((4,))],
        compiler_params=pltpu.CompilerParams(collective_id=0, has_side_effects=True, vmem_limit_bytes=60 << 20),
        cost_estimate=pl.CostEstimate(flops=2 * 512 * D * 2560, bytes_accessed=30 << 20, transcendentals=0),
        name="qkv",
    )(hn, cos, sin, qg, kg, wq, wk, wv)


SEQ = 4
PER = ROWS // SEQ


def attn_kernel(pos, q, kc, vc, kn, vn, kn_src, vn_src, o_rx, kn_rx, vn_rx,
                oscr, osend, so, ro, sk, rk, sv, rv, lsem):
    step = pl.program_id(0)
    me = lax.axis_index("x")
    c1, c2, c3 = partners(me)
    order = (c2, c3, c1, me)

    def o_copy(k):
        return remote(osend.at[k], o_rx.at[pl.ds(me * 4, 4)], so.at[k], ro.at[k], order[k])

    def n_copy(k, src, dst, ss, rs):
        return remote(src.at[pl.ds(order[k] * ROWS, ROWS)], dst.at[:, :, me], ss.at[k], rs.at[k], order[k])

    def own_copies():
        return (pltpu.make_async_copy(osend.at[3], o_rx.at[pl.ds(me * 4, 4)], lsem.at[0]),
                pltpu.make_async_copy(kn_src.at[pl.ds(me * ROWS, ROWS)], kn_rx.at[:, :, me], lsem.at[1]),
                pltpu.make_async_copy(vn_src.at[pl.ds(me * ROWS, ROWS)], vn_rx.at[:, :, me], lsem.at[2]))

    @pl.when(step == 0)
    def _():
        greet((c1, c2, c3))
        for k in range(3):
            n_copy(k, kn_src, kn_rx, sk, rk).start()
            n_copy(k, vn_src, vn_rx, sv, rv).start()
        own_copies()[1].start()
        own_copies()[2].start()

    for k in range(3):
        @pl.when(step == (k + 1) * PER)
        def _(k=k):
            o_copy(k).start()

    which = step // PER
    dest = jnp.where(which == 0, c2, jnp.where(which == 1, c3, jnp.where(which == 2, c1, me)))
    base = dest * ROWS + lax.rem(step, PER) * SEQ
    row = lax.broadcasted_iota(jnp.int32, (64, 2 * T), 0)
    col = lax.broadcasted_iota(jnp.int32, (64, 2 * T), 1)
    same_head = lax.rem(row // 8, 2) == lax.rem(col, 2)
    nrow = lax.broadcasted_iota(jnp.int32, (64, 8), 0)
    ncol = lax.broadcasted_iota(jnp.int32, (64, 8), 1)
    new_ok = (lax.rem(nrow // 8, 2) == lax.rem(ncol, 2)) & (ncol // 2 <= nrow // 16)
    scale = HD ** -0.5
    dims = (((1,), (1,)), ((), ()))
    for i in range(SEQ):
        start = pos[base + i]
        q2 = q[:, i].reshape(64, HD)
        s_old = lax.dot_general(q2, kc[i], dims, preferred_element_type=F32) * scale
        s_old = jnp.where(same_head & (col < 2 * start), s_old, -jnp.inf)
        s_new = lax.dot_general(q2, kn[i], dims, preferred_element_type=F32) * scale
        s_new = jnp.where(new_ok, s_new, -jnp.inf)
        peak = jnp.maximum(jnp.max(s_old, axis=-1, keepdims=True), jnp.max(s_new, axis=-1, keepdims=True))
        w_old = jnp.exp(s_old - peak)
        w_new = jnp.exp(s_new - peak)
        total = jnp.sum(w_old, axis=-1, keepdims=True) + jnp.sum(w_new, axis=-1, keepdims=True)
        mixed = jnp.dot(w_old.astype(BF16), vc[i], preferred_element_type=F32)
        mixed = mixed + jnp.dot(w_new.astype(BF16), vn[i], preferred_element_type=F32)
        oscr[pl.ds(lax.rem(step, PER) * SEQ + i, 64, stride=ROWS), :] = mixed / total

    @pl.when(lax.rem(step, PER) == PER - 1)
    def _():
        for s in range(STEPS):
            for hg in range(QH):
                osend[which, hg // 4, s * ROWS:(s + 1) * ROWS, (hg % 4) * HD:(hg % 4 + 1) * HD] = (
                    oscr[pl.ds((s * QH + hg) * ROWS, ROWS), :].astype(BF16))

    @pl.when(step == 4 * PER - 1)
    def _():
        own_copies()[0].start()
        for cp in own_copies():
            cp.wait()
        for k in range(3):
            o_copy(k).wait()
            n_copy(k, kn_src, kn_rx, sk, rk).wait()
            n_copy(k, vn_src, vn_rx, sv, rv).wait()


def attention(pos, q, kc, vc, kn, vn):
    hbm = pl.BlockSpec(memory_space=pl.ANY)
    dma = pltpu.SemaphoreType.DMA

    def block(step):
        me = lax.axis_index("x")
        c1, c2, c3 = partners(me)
        which = step // PER
        dest = jnp.where(which == 0, c2, jnp.where(which == 1, c3, jnp.where(which == 2, c1, me)))
        return dest * PER + lax.rem(step, PER)

    seq = lambda rows: pl.BlockSpec((SEQ, rows, HD), lambda i: (block(i), 0, 0))
    new = jax.ShapeDtypeStruct((ROWS, STEPS, 4, 2, HD), BF16)
    return pl.pallas_call(
        attn_kernel,
        grid=(4 * PER,),
        out_shape=(jax.ShapeDtypeStruct((16, TOK, 512), BF16), new, new),
        in_specs=[pl.BlockSpec(memory_space=pltpu.SMEM),
                  pl.BlockSpec((STEPS, SEQ, QH, HD), lambda i: (0, block(i), 0, 0)),
                  seq(2 * T), seq(2 * T), seq(8), seq(8), hbm, hbm],
        out_specs=(hbm,) * 3,
        scratch_shapes=[
            pltpu.VMEM((64 * ROWS, HD), F32), pltpu.VMEM((4, 4, TOK, 512), BF16),
            dma((3,)), dma((3,)), dma((3,)), dma((3,)), dma((3,)), dma((3,)), dma((3,))],
        compiler_params=pltpu.CompilerParams(collective_id=1, has_side_effects=True, vmem_limit_bytes=40 << 20),
        cost_estimate=pl.CostEstimate(flops=4 * 128 * 64 * 512 * 128, bytes_accessed=36 << 20, transcendentals=0),
        name="attention",
    )(pos, q, kc.reshape(GROUP, 2 * T, HD), vc.reshape(GROUP, 2 * T, HD), kn, vn,
      kn.reshape(GROUP, STEPS, 2, HD), vn.reshape(GROUP, STEPS, 2, HD))


NB = 3
N_O = 16
N_C = FF // 256
N_D = FF // 512


def mlp_kernel(o, hid, gain, wo, wg, wu, wd, kc, vc, out, k_rx, v_rx,
               wrow, wcol, acc, x1, z, g, rsem, csem, ks, kr, vs, vr):
    me = lax.axis_index("x")
    c1, c2, c3 = partners(me)
    order = (c2, c3, c1)

    def row_o(i):
        slot = lax.rem(i, NB)
        return pltpu.make_async_copy(wo.at[pl.ds(i * 512, 512)], wrow.at[slot], rsem.at[slot])

    def row_d(i):
        slot = lax.rem(i + N_O, NB)
        return pltpu.make_async_copy(wd.at[pl.ds(i * 512, 512)], wrow.at[slot], rsem.at[slot])

    def col(i):
        slot = lax.rem(i, NB)
        at = pl.ds(pl.multiple_of(i * 256, 256), 256)
        return (pltpu.make_async_copy(wg.at[:, at], wcol.at[slot, 0], csem.at[slot, 0]),
                pltpu.make_async_copy(wu.at[:, at], wcol.at[slot, 1], csem.at[slot, 1]))

    for i in range(NB):
        row_o(i).start()
    greet((c1, c2, c3))
    bulk = []
    for k in range(3):
        for src, dst, ss, rs in ((kc, k_rx, ks, kr), (vc, v_rx, vs, vr)):
            bulk.append(remote(src.at[pl.ds(order[k] * ROWS, ROWS)], dst.at[k], ss.at[k], rs.at[k], order[k]))
    for cp in bulk:
        cp.start()
    for i in range(NB):
        for cp in col(i):
            cp.start()

    def accumulate(lhs, slot, first):
        for n in range(10):
            cols = slice(n * 512, (n + 1) * 512)
            part = jnp.dot(lhs, wrow[slot, :, cols], preferred_element_type=F32)
            acc[:, cols] = acc[:, cols] + part

    acc[...] = jnp.zeros_like(acc)

    def o_step(i, carry):
        row_o(i).wait()
        accumulate(o[i], lax.rem(i, NB), i == 0)

        @pl.when(i + NB < N_O)
        def _():
            row_o(i + NB).start()

        @pl.when(i + NB >= N_O)
        def _():
            row_d(i + NB - N_O).start()
        return carry

    lax.fori_loop(0, N_O, o_step, 0)

    def norm_step(r, carry):
        rows = pl.ds(r * 16, 16)
        res = (hid[rows, :].astype(F32) + acc[rows, :]).astype(BF16)
        x1[rows, :] = res
        res = res.astype(F32)
        inv = lax.rsqrt(jnp.mean(res * res, axis=-1, keepdims=True) + EPS)
        z[rows, :] = (res * inv * gain[...]).astype(BF16)
        acc[rows, :] = jnp.zeros((16, D), F32)
        return carry

    lax.fori_loop(0, TOK // 16, norm_step, 0)

    def col_step(i, carry):
        slot = lax.rem(i, NB)
        for cp in col(i):
            cp.wait()
        gate = jnp.dot(z[...], wcol[slot, 0], preferred_element_type=F32)
        up = jnp.dot(z[...], wcol[slot, 1], preferred_element_type=F32)
        g[i // 2, :, pl.ds(pl.multiple_of(lax.rem(i, 2) * 256, 256), 256)] = (
            gate * jax.nn.sigmoid(gate) * up).astype(BF16)

        @pl.when(i + NB < N_C)
        def _():
            for cp in col(i + NB):
                cp.start()
        return carry

    lax.fori_loop(0, N_C, col_step, 0)

    def d_step(i, carry):
        row_d(i).wait()
        accumulate(g[i], lax.rem(i + N_O, NB), i == 0)

        @pl.when(i + NB < N_D)
        def _():
            row_d(i + NB).start()
        return carry

    lax.fori_loop(0, N_D, d_step, 0)

    def out_step(r, carry):
        rows = pl.ds(r * 16, 16)
        out[rows, :] = (x1[rows, :].astype(F32) + acc[rows, :]).astype(BF16)
        return carry

    lax.fori_loop(0, TOK // 16, out_step, 0)
    for cp in bulk:
        cp.wait()


def mlp(o, hid, gain, wo, wg, wu, wd, kc, vc):
    vmem = pl.BlockSpec(memory_space=pltpu.VMEM)
    hbm = pl.BlockSpec(memory_space=pl.ANY)
    dma = pltpu.SemaphoreType.DMA
    rx = jax.ShapeDtypeStruct((3, ROWS, T, 2, HD), BF16)
    return pl.pallas_call(
        mlp_kernel,
        out_shape=(jax.ShapeDtypeStruct((TOK, D), BF16), rx, rx),
        in_specs=[vmem] * 3 + [hbm] * 6,
        out_specs=(vmem, hbm, hbm),
        scratch_shapes=[
            pltpu.VMEM((NB, 512, D), BF16), pltpu.VMEM((NB, 2, D, 256), BF16),
            pltpu.VMEM((TOK, D), F32), pltpu.VMEM((TOK, D), BF16), pltpu.VMEM((TOK, D), BF16),
            pltpu.VMEM((N_D, TOK, 512), BF16),
            dma((NB,)), dma((NB, 2)), dma((3,)), dma((3,)), dma((3,)), dma((3,))],
        compiler_params=pltpu.CompilerParams(collective_id=2, has_side_effects=True, vmem_limit_bytes=60 << 20),
        cost_estimate=pl.CostEstimate(flops=2 * TOK * D * (8192 + 3 * FF), bytes_accessed=900 << 20, transcendentals=0),
        name="mlp",
    )(o, hid, gain, wo, wg, wu, wd, kc, vc)


AB = 2
AR = 4


def place_kernel(pos, kc, vc, k_rx, v_rx, kn, vn, k_out, v_out, kbuf, vbuf, isem, osem):
    me = lax.axis_index("x")
    c1, c2, c3 = partners(me)
    n_pieces = ROWS // AB
    arrays = ((kc, k_rx, kn, k_out, kbuf), (vc, v_rx, vn, v_out, vbuf))

    def loads(i):
        slot = lax.rem(i, AR)
        copies = []
        for a, (own, rx, _, _, buf) in enumerate(arrays):
            for k, dev in enumerate((c2, c3, c1)):
                copies.append(pltpu.make_async_copy(
                    rx.at[k, pl.ds(i * AB, AB)], buf.at[slot, :, :, dev], isem.at[slot, a, k]))
            copies.append(pltpu.make_async_copy(
                own.at[pl.ds(me * ROWS + i * AB, AB)], buf.at[slot, :, :, me], isem.at[slot, a, 3]))
        return copies

    def stores(i):
        slot = lax.rem(i, AR)
        return [pltpu.make_async_copy(buf.at[slot], out.at[pl.ds(i * AB, AB)], osem.at[slot, a])
                for a, (_, _, _, out, buf) in enumerate(arrays)]

    for i in range(AR - 1):
        for cp in loads(i):
            cp.start()

    def piece(i, carry):
        slot = lax.rem(i, AR)
        for cp in loads(i):
            cp.wait()
        for b in range(AB):
            start = pos[i * AB + b]
            for _, _, new, _, buf in arrays:
                for s in range(STEPS):
                    buf[slot, b, start + s] = new[i * AB + b, s]
        for cp in stores(i):
            cp.start()

        @pl.when(i >= 1)
        def _():
            for cp in stores(i - 1):
                cp.wait()

        @pl.when(i + AR - 1 < n_pieces)
        def _():
            for cp in loads(i + AR - 1):
                cp.start()
        return carry

    lax.fori_loop(0, n_pieces, piece, 0)
    for cp in stores(n_pieces - 1):
        cp.wait()


def place(pos, kc, vc, k_rx, v_rx, kn, vn):
    hbm = pl.BlockSpec(memory_space=pl.ANY)
    vmem = pl.BlockSpec(memory_space=pltpu.VMEM)
    out = jax.ShapeDtypeStruct((ROWS, T, 4, 2, HD), BF16)
    buf = pltpu.VMEM((AR, AB, T, 4, 2, HD), BF16)
    dma = pltpu.SemaphoreType.DMA
    return pl.pallas_call(
        place_kernel,
        out_shape=(out, out),
        in_specs=[pl.BlockSpec(memory_space=pltpu.SMEM)] + [hbm] * 4 + [vmem] * 2,
        out_specs=(hbm, hbm),
        scratch_shapes=[buf, buf, dma((AR, 2, 4)), dma((AR, 2))],
        compiler_params=pltpu.CompilerParams(vmem_limit_bytes=40 << 20),
        cost_estimate=pl.CostEstimate(flops=1 << 20, bytes_accessed=68 << 20, transcendentals=0),
        name="place",
    )(pos, kc, vc, k_rx, v_rx, kn, vn)


def solution(mesh):
    row_spec = P(None, ('dp', 'x'), None)
    cache_in = P('dp', None, 'x', None)
    cache_out = P(('dp', 'x'), None, None, None)

    def local_run(start_pos, hidden_in, k_heads, v_heads, attn_norm, w_q, w_k, w_v, q_norm, k_norm, w_o, mlp_norm, w_gate, w_up, w_down):
        my_pos = lax.dynamic_slice_in_dim(start_pos, lax.axis_index('x') * ROWS, ROWS)
        hid = hidden_in.reshape(TOK, D)
        hn = rms_norm(hid, attn_norm).astype(BF16)

        inv_freq = jnp.power(THETA, -jnp.arange(HD // 2, dtype=F32) * 2.0 / HD)
        positions = start_pos.reshape(4, 1, ROWS) + jnp.arange(STEPS)[None, :, None]
        angles = positions.astype(F32)[..., None] * inv_freq
        cos = jnp.cos(angles)
        sin = jnp.sin(angles)
        cos = jnp.concatenate([cos, cos], axis=-1).reshape(16, ROWS, HD)
        sin = jnp.concatenate([-sin, sin], axis=-1).reshape(16, ROWS, HD)

        q, kn, vn = qkv(hn, cos, sin, q_norm.astype(F32)[None], k_norm.astype(F32)[None], w_q, w_k, w_v)
        o, kn_rx, vn_rx = attention(start_pos, q, k_heads, v_heads, kn, vn)
        out, k_rx, v_rx = mlp(o, hid, mlp_norm.astype(F32)[None], w_o, w_gate, w_up, w_down, k_heads, v_heads)
        k_out, v_out = place(my_pos, k_heads, v_heads, k_rx, v_rx, kn_rx, vn_rx)
        return (out.reshape(STEPS, ROWS, D), k_out.reshape(ROWS, T, 8, HD), v_out.reshape(ROWS, T, 8, HD))

    return jax.shard_map(local_run, mesh=mesh, in_specs=(P('dp'), row_spec, cache_in, cache_in) + (P(),) * 11, out_specs=(row_spec, cache_out, cache_out), check_vma=False)
```

```python
import jax
import jax.numpy as jnp
from jax import lax
from jax.experimental import pallas as pl
from jax.experimental.pallas import tpu as pltpu
from jax.sharding import PartitionSpec as P

EPS = 1e-6
THETA = 1000000.0
F32 = jnp.float32
BF16 = jnp.bfloat16
MESH = pl.DeviceIdType.MESH

STEPS = 4
ROWS = 32
TOK = STEPS * ROWS
GROUP = 128
D = 5120
HD = 128
QH = 16
FF = 25600
T = 256
SEQ = 4
PER = ROWS // SEQ
NS = 2
NR = 4
NC = 5
N_O = 32
N_C = FF // 256
N_D = FF // 256
PARTS = ((0, 2), (2, 1), (3, 1), (4, 1), (5, 27))


def partners(me):
    c1 = me + 1 - 2 * lax.rem(me, 2)
    c2 = lax.rem(me + 2, 4)
    c3 = 3 - me
    return c1, c2, c3


def greet(devices):
    barrier = pltpu.get_barrier_semaphore()
    for dev in devices:
        pl.semaphore_signal(barrier, inc=1, device_id={"x": dev}, device_id_type=MESH)
    pl.semaphore_wait(barrier, len(devices))


def remote(src, dst, ssem, rsem, dev):
    return pltpu.make_async_remote_copy(
        src_ref=src, dst_ref=dst, send_sem=ssem, recv_sem=rsem,
        device_id={"x": dev}, device_id_type=MESH)


def block_copies(kc, vc, k_rx, v_rx, sems, me, first, count, at):
    ks, kr, vs, vr = sems
    copies = []
    for k, dev in ((1, (me + 2) % 4), (2, 3 - me), (0, partners(me)[0])):
        rows = pl.ds(dev * ROWS + first, count)
        for src, dst, ss, rs in ((kc, k_rx, ks, kr), (vc, v_rx, vs, vr)):
            copies.append(remote(src.at[rows], dst.at[k, pl.ds(at, count)], ss.at[k], rs.at[k], dev))
    return copies


def layer_kernel(pos, gain, gain2, cos, sin, qg, kg, hid, wq, wk, wv, wo, wg, wu, wd, kc, vc, kc2, vc2,
                 out, kn_rx, vn_rx, k_rx, v_rx,
                 ws, wrow, hall, hn, tscr, kscr, vscr, q, kn, vn, kbuf, vbuf, o_rx, acc,
                 wsem, osem, s1, r1, s2, r2, sf, rf, kvsem, so, ro, sk, rk, sv, rv, lsem,
                 rsem, csem, ks, kr, vs, vr):
    me = lax.axis_index("x")
    c1, c2, c3 = partners(me)
    order = (c2, c3, c1, me)

    def bulk(part):
        first, count = PARTS[part]
        return block_copies(kc, vc, k_rx, v_rx, [sem.at[part] for sem in (ks, kr, vs, vr)], me, first, count, first)

    def start_bulk(part):
        for cp in bulk(part):
            cp.start()

    def row_o(i):
        slot = lax.rem(i, NR)
        return pltpu.make_async_copy(wo.at[pl.ds(i * 256, 256)], wrow.at[slot], rsem.at[slot])

    def row_d(i):
        slot = lax.rem(i + N_O, NR)
        return pltpu.make_async_copy(wd.at[pl.ds(i * 256, 256)], wrow.at[slot], rsem.at[slot])

    def col(i):
        slot = lax.rem(i, NC)
        at = pl.ds(pl.multiple_of(i * 256, 256), 256)
        return (pltpu.make_async_copy(wg.at[:, at], ws.at[2 * slot], csem.at[slot, 0]),
                pltpu.make_async_copy(wu.at[:, at], ws.at[2 * slot + 1], csem.at[slot, 1]))

    def owner(step):
        which = step // PER
        return jnp.where(which == 0, c2, jnp.where(which == 1, c3, jnp.where(which == 2, c1, me)))

    def base_of(step):
        return owner(step) * ROWS + lax.rem(step, PER) * SEQ

    def kv_loads(step):
        slot = lax.rem(step, NS)
        rows = pl.ds(base_of(step), SEQ)
        return (pltpu.make_async_copy(kc2.at[rows], kbuf.at[slot], kvsem.at[slot, 0]),
                pltpu.make_async_copy(vc2.at[rows], vbuf.at[slot], kvsem.at[slot, 1]))

    wcopies = []
    for c in range(10):
        if c < 8:
            src = wq.at[:, pl.ds(pl.multiple_of(me * 2048 + c * 256, 256), 256)]
        else:
            src = (wk if c == 8 else wv).at[:, pl.ds(pl.multiple_of(me * 256, 256), 256)]
        wcopies.append(pltpu.make_async_copy(src, ws.at[c], wsem.at[c]))

    greet((c1, c2, c3))
    cross = []
    fwd = []
    for s in range(STEPS):
        row = 256 + (s // 2) * 128 + (s % 2) * 32
        cross.append(remote(hid.at[pl.ds(s * 32, 32)], hall.at[pl.ds(row, 32)], s2.at[s], r2.at[s], c2))
        fwd.append(remote(hall.at[pl.ds(row, 32)], hall.at[pl.ds(row + 64, 32)], sf.at[s], rf.at[s], c1))
    for cp in cross:
        cp.start()
    near = remote(hid, hall.at[pl.ds(128, 128)], s1, r1, c1)
    near.start()
    own = pltpu.make_async_copy(hid, hall.at[pl.ds(0, 128)], osem)
    own.start()
    for cp in wcopies:
        cp.start()
    start_bulk(0)
    for step in range(NS):
        for cp in kv_loads(step):
            cp.start()
    for i in range(NR):
        row_o(i).start()

    def table(ref, groups):
        return jnp.concatenate([ref[j * STEPS + s] for j, s in groups], axis=0)

    for blk in range(4):
        if blk == 0:
            own.wait()
            groups = [(me, s) for s in range(4)]
        elif blk == 1:
            near.wait_recv()
            groups = [(c1, s) for s in range(4)]
        else:
            lo = (blk - 2) * 2
            for s in (lo, lo + 1):
                cross[s].wait_recv()
                fwd[s].start()
            for s in (lo, lo + 1):
                fwd[s].wait_recv()
            groups = [(c2, lo), (c2, lo + 1), (c3, lo), (c3, lo + 1)]

        def norm_step(r, carry, blk=blk):
            val = hall[pl.ds(blk * 128 + r * 16, 16), :].astype(F32)
            inv = lax.rsqrt(jnp.mean(val * val, axis=-1, keepdims=True) + EPS)
            hn[pl.ds(r * 16, 16), :] = (val * inv * gain[...]).astype(BF16)
            return carry

        lax.fori_loop(0, 8, norm_step, 0)
        cos_b = table(cos, groups)
        sin_b = table(sin, groups)

        def head(val, head_gain, cos_b=cos_b, sin_b=sin_b):
            inv = lax.rsqrt(jnp.mean(val * val, axis=-1, keepdims=True) + EPS)
            val = val * inv * head_gain
            return val * cos_b + pltpu.roll(val, 64, 1) * sin_b

        def project(c):
            return jnp.dot(hn[...], ws[c], preferred_element_type=F32)

        def q_chunk(c, carry, head=head):
            val = project(c)
            for hh in range(2):
                tscr[pl.ds(2 * c + hh, 128, stride=QH), :] = head(val[:, hh * HD:(hh + 1) * HD], qg[...])
            return carry

        if blk == 0:
            for cp in wcopies:
                cp.wait()
        lax.fori_loop(0, 8, q_chunk, 0)
        k_acc = project(8)
        v_acc = project(9)
        for hh in range(2):
            k_head = head(k_acc[:, hh * HD:(hh + 1) * HD], kg[...])
            v_head = v_acc[:, hh * HD:(hh + 1) * HD]
            for g, (j, s) in enumerate(groups):
                at = pl.ds(j * 256 + s * 2 + hh, 32, stride=8)
                kscr[at, :] = k_head[g * 32:(g + 1) * 32]
                vscr[at, :] = v_head[g * 32:(g + 1) * 32]
        for g, (j, s) in enumerate(groups):
            q[s, pl.ds(j * 32, 32)] = tscr[pl.ds(g * 512, 512), :].reshape(32, QH, HD).astype(BF16)
    kn[...] = kscr[...].reshape(GROUP, 8, HD).astype(BF16)
    vn[...] = vscr[...].reshape(GROUP, 8, HD).astype(BF16)
    for s in range(STEPS):
        cross[s].wait_send()
        fwd[s].wait_send()
    near.wait_send()

    def o_copy(k):
        return remote(hall.at[pl.ds(k * TOK, TOK), pl.ds(0, 2048)],
                      o_rx.at[:, pl.ds(pl.multiple_of(me * 2048, 2048), 2048)], so.at[k], ro.at[k], order[k])

    def n_copies(k):
        rows = pl.ds(order[k] * ROWS, ROWS)
        return (remote(kn.at[rows], kn_rx.at[me], sk.at[k], rk.at[k], order[k]),
                remote(vn.at[rows], vn_rx.at[me], sv.at[k], rv.at[k], order[k]))

    own_rows = pl.ds(me * ROWS, ROWS)
    own_new = (pltpu.make_async_copy(kn.at[own_rows], kn_rx.at[me], lsem.at[0]),
               pltpu.make_async_copy(vn.at[own_rows], vn_rx.at[me], lsem.at[1]))

    row = lax.broadcasted_iota(jnp.int32, (64, 2 * T), 0)
    lane = lax.broadcasted_iota(jnp.int32, (64, 2 * T), 1)
    same_head = lax.rem(row // 8, 2) == lax.rem(lane, 2)
    nrow = lax.broadcasted_iota(jnp.int32, (64, 8), 0)
    nlane = lax.broadcasted_iota(jnp.int32, (64, 8), 1)
    new_ok = (lax.rem(nrow // 8, 2) == lax.rem(nlane, 2)) & (nlane // 2 <= nrow // 16)
    scale = HD ** -0.5
    dims = (((1,), (1,)), ((), ()))

    for k in range(4):
        def attend(j, carry, k=k):
            step = k * PER + j
            slot = lax.rem(step, NS)
            base = base_of(step)
            for cp in kv_loads(step):
                cp.wait()
            for i in range(SEQ):
                start = pos[base + i]
                q2 = q[:, base + i].reshape(64, HD)
                s_old = lax.dot_general(q2, kbuf[slot, i], dims, preferred_element_type=F32) * scale
                s_old = jnp.where(same_head & (lane < 2 * start), s_old, -jnp.inf)
                s_new = lax.dot_general(q2, kn[base + i], dims, preferred_element_type=F32) * scale
                s_new = jnp.where(new_ok, s_new, -jnp.inf)
                peak = jnp.maximum(jnp.max(s_old, axis=-1, keepdims=True), jnp.max(s_new, axis=-1, keepdims=True))
                w_old = jnp.exp(s_old - peak)
                w_new = jnp.exp(s_new - peak)
                total = jnp.sum(w_old, axis=-1, keepdims=True) + jnp.sum(w_new, axis=-1, keepdims=True)
                mixed = jnp.dot(w_old.astype(BF16), vbuf[slot, i], preferred_element_type=F32)
                mixed = mixed + jnp.dot(w_new.astype(BF16), vn[base + i], preferred_element_type=F32)
                tscr[pl.ds(j * SEQ + i, 64, stride=ROWS), :] = mixed / total

            @pl.when(step + NS < 4 * PER)
            def _():
                for cp in kv_loads(step + NS):
                    cp.start()

            @pl.when(j == 1)
            def _():
                if k == 0:
                    for kk in range(3):
                        for cp in n_copies(kk):
                            cp.start()
                    for cp in own_new:
                        cp.start()
                    start_bulk(1)
                else:
                    o_copy(k - 1).start()
                    start_bulk(k + 1)
            return carry

        if k == 0:
            for i in range(NC):
                for cp in col(i):
                    cp.start()
        lax.fori_loop(0, PER, attend, 0)
        for s in range(STEPS):
            for hg in range(QH):
                val = tscr[pl.ds((s * QH + hg) * ROWS, ROWS), :].astype(BF16)
                if k < 3:
                    hall[k * TOK + s * ROWS:k * TOK + (s + 1) * ROWS, hg * HD:(hg + 1) * HD] = val
                else:
                    o_rx[s * ROWS:(s + 1) * ROWS, pl.ds(pl.multiple_of(me * 2048 + hg * HD, HD), HD)] = val

    acc[...] = jnp.zeros_like(acc)
    for k in (2, 0, 1):
        o_copy(k).wait()

    def accumulate(lhs, slot):
        for n in range(10):
            cols = slice(n * 512, (n + 1) * 512)
            acc[:, cols] = acc[:, cols] + jnp.dot(lhs, wrow[slot, :, cols], preferred_element_type=F32)

    def o_step(i, carry):
        row_o(i).wait()
        accumulate(o_rx[:, pl.ds(pl.multiple_of(i * 256, 256), 256)], lax.rem(i, NR))

        @pl.when(i + NR < N_O)
        def _():
            row_o(i + NR).start()

        @pl.when(i + NR >= N_O)
        def _():
            row_d(i + NR - N_O).start()
        return carry

    lax.fori_loop(0, N_O, o_step, 0)

    def norm2_step(r, carry):
        rows = pl.ds(r * 16, 16)
        res = (hid[rows, :].astype(F32) + acc[rows, :]).astype(BF16)
        out[rows, :] = res
        res = res.astype(F32)
        inv = lax.rsqrt(jnp.mean(res * res, axis=-1, keepdims=True) + EPS)
        hn[rows, :] = (res * inv * gain2[...]).astype(BF16)
        acc[rows, :] = jnp.zeros((16, D), F32)
        return carry

    lax.fori_loop(0, TOK // 16, norm2_step, 0)

    def act_at(i):
        return pl.ds((i // 20) * 128, 128), pl.ds(pl.multiple_of(lax.rem(i, 20) * 256, 256), 256)

    def col_step(i, carry):
        slot = lax.rem(i, NC)
        for cp in col(i):
            cp.wait()
        gate = jnp.dot(hn[...], ws[2 * slot], preferred_element_type=F32)
        up = jnp.dot(hn[...], ws[2 * slot + 1], preferred_element_type=F32)
        rows, cols = act_at(i)
        hall[rows, cols] = (gate * jax.nn.sigmoid(gate) * up).astype(BF16)

        @pl.when(i + NC < N_C)
        def _():
            for cp in col(i + NC):
                cp.start()
        return carry

    lax.fori_loop(0, N_C, col_step, 0)

    def d_step(i, carry):
        row_d(i).wait()
        rows, cols = act_at(i)
        accumulate(hall[rows, cols], lax.rem(i + N_O, NR))

        @pl.when(i + NR < N_D)
        def _():
            row_d(i + NR).start()
        return carry

    lax.fori_loop(0, N_D, d_step, 0)

    def out_step(r, carry):
        rows = pl.ds(r * 16, 16)
        out[rows, :] = (out[rows, :].astype(F32) + acc[rows, :]).astype(BF16)
        return carry

    lax.fori_loop(0, TOK // 16, out_step, 0)
    for k in range(3):
        for cp in n_copies(k):
            cp.wait()
    for cp in own_new:
        cp.wait()
    for part in range(len(PARTS)):
        for cp in bulk(part):
            cp.wait()


def layer(pos, gain, gain2, cos, sin, qg, kg, hid, wq, wk, wv, wo, wg, wu, wd, kc, vc):
    vmem = pl.BlockSpec(memory_space=pltpu.VMEM)
    hbm = pl.BlockSpec(memory_space=pl.ANY)
    dma = pltpu.SemaphoreType.DMA
    new = jax.ShapeDtypeStruct((4, ROWS, 8, HD), BF16)
    rx = jax.ShapeDtypeStruct((3, ROWS, T, 2, HD), BF16)
    n_parts = len(PARTS)
    return pl.pallas_call(
        layer_kernel,
        out_shape=(jax.ShapeDtypeStruct((TOK, D), BF16), new, new, rx, rx),
        in_specs=[pl.BlockSpec(memory_space=pltpu.SMEM)] + [vmem] * 7 + [hbm] * 11,
        out_specs=(vmem,) + (hbm,) * 4,
        scratch_shapes=[
            pltpu.VMEM((10, D, 256), BF16),
            pltpu.VMEM((NR, 256, D), BF16),
            pltpu.VMEM((640, D), BF16),
            pltpu.VMEM((TOK, D), BF16),
            pltpu.VMEM((2048, HD), F32),
            pltpu.VMEM((GROUP * 8, HD), F32), pltpu.VMEM((GROUP * 8, HD), F32),
            pltpu.VMEM((STEPS, GROUP, QH, HD), BF16),
            pltpu.VMEM((GROUP, 8, HD), BF16), pltpu.VMEM((GROUP, 8, HD), BF16),
            pltpu.VMEM((NS, SEQ, 2 * T, HD), BF16), pltpu.VMEM((NS, SEQ, 2 * T, HD), BF16),
            pltpu.VMEM((TOK, 8192), BF16),
            pltpu.VMEM((TOK, D), F32),
            dma((10,)), dma, dma, dma, dma((4,)), dma((4,)), dma((4,)), dma((4,)), dma((NS, 2)),
            dma((3,)), dma((3,)), dma((3,)), dma((3,)), dma((3,)), dma((3,)), dma((2,)),
            dma((NR,)), dma((NC, 2)),
            dma((n_parts, 3)), dma((n_parts, 3)), dma((n_parts, 3)), dma((n_parts, 3))],
        compiler_params=pltpu.CompilerParams(collective_id=0, has_side_effects=True, vmem_limit_bytes=67043328),
        cost_estimate=pl.CostEstimate(flops=2 * TOK * D * (18432 + 3 * FF), bytes_accessed=1000 << 20, transcendentals=0),
        name="layer",
    )(pos, gain, gain2, cos, sin, qg, kg, hid, wq, wk, wv, wo, wg, wu, wd, kc, vc,
      kc.reshape(GROUP, 2 * T, HD), vc.reshape(GROUP, 2 * T, HD))


AR = 8


def place_kernel(pos, kc, vc, k_rx, v_rx, kn, vn, k_out, v_out, kbuf, vbuf, isem, osem):
    me = lax.axis_index("x")
    c1, c2, c3 = partners(me)
    arrays = ((kc, k_rx, kn, k_out, kbuf), (vc, v_rx, vn, v_out, vbuf))

    def loads(i):
        slot = i % AR
        copies = []
        for a, (own, rx, _, _, buf) in enumerate(arrays):
            for k, dev in enumerate((c1, c2, c3)):
                copies.append(pltpu.make_async_copy(
                    rx.at[k, i], buf.at[slot, :, dev], isem.at[slot, a, k]))
            copies.append(pltpu.make_async_copy(
                own.at[me * ROWS + i], buf.at[slot, :, me], isem.at[slot, a, 3]))
        return copies

    def stores(i):
        slot = i % AR
        return [pltpu.make_async_copy(buf.at[slot], out.at[i], osem.at[slot, a])
                for a, (_, _, _, out, buf) in enumerate(arrays)]

    incoming = {}
    outgoing = {}
    for i in range(AR - 2):
        incoming[i] = loads(i)
        for cp in incoming[i]:
            cp.start()
    for i in range(ROWS):
        for cp in incoming[i]:
            cp.wait()
        start = pos[i]
        for _, _, new, _, buf in arrays:
            for s in range(STEPS):
                for x in range(4):
                    buf[i % AR, start + s, x] = new[x, i, s]
        outgoing[i] = stores(i)
        for cp in outgoing[i]:
            cp.start()
        if i >= 2:
            for cp in outgoing[i - 2]:
                cp.wait()
        nxt = i + AR - 2
        if nxt < ROWS:
            incoming[nxt] = loads(nxt)
            for cp in incoming[nxt]:
                cp.start()
    for i in (ROWS - 2, ROWS - 1):
        for cp in outgoing[i]:
            cp.wait()


def place(pos, kc, vc, k_rx, v_rx, kn, vn):
    hbm = pl.BlockSpec(memory_space=pl.ANY)
    vmem = pl.BlockSpec(memory_space=pltpu.VMEM)
    out = jax.ShapeDtypeStruct((ROWS, T, 4, 2, HD), BF16)
    buf = pltpu.VMEM((AR, T, 4, 2, HD), BF16)
    dma = pltpu.SemaphoreType.DMA
    return pl.pallas_call(
        place_kernel,
        out_shape=(out, out),
        in_specs=[pl.BlockSpec(memory_space=pltpu.SMEM)] + [hbm] * 4 + [vmem] * 2,
        out_specs=(hbm, hbm),
        scratch_shapes=[buf, buf, dma((AR, 2, 4)), dma((AR, 2))],
        compiler_params=pltpu.CompilerParams(vmem_limit_bytes=60 << 20),
        cost_estimate=pl.CostEstimate(flops=1 << 20, bytes_accessed=68 << 20, transcendentals=0),
        name="place",
    )(pos, kc, vc, k_rx, v_rx, kn.reshape(4, ROWS, STEPS, 2, HD), vn.reshape(4, ROWS, STEPS, 2, HD))


def solution(mesh):
    row_spec = P(None, ('dp', 'x'), None)
    cache_in = P('dp', None, 'x', None)
    cache_out = P(('dp', 'x'), None, None, None)

    def local_run(start_pos, hidden_in, k_heads, v_heads, attn_norm, w_q, w_k, w_v, q_norm, k_norm, w_o, mlp_norm, w_gate, w_up, w_down):
        my_pos = lax.dynamic_slice_in_dim(start_pos, lax.axis_index('x') * ROWS, ROWS)
        hid = hidden_in.reshape(TOK, D)

        half = jnp.power(THETA, -jnp.arange(HD // 2, dtype=F32) * 2.0 / HD)
        inv_freq = jnp.concatenate([half, half])
        sign = jnp.where(jnp.arange(HD) < HD // 2, -1.0, 1.0).astype(F32)
        positions = start_pos.reshape(4, 1, ROWS) + jnp.arange(STEPS)[None, :, None]
        angles = positions.astype(F32)[..., None] * inv_freq
        cos = jnp.cos(angles).reshape(16, ROWS, HD)
        sin = (jnp.sin(angles) * sign).reshape(16, ROWS, HD)

        out, kn, vn, k_rx, v_rx = layer(
            start_pos, attn_norm.astype(F32)[None], mlp_norm.astype(F32)[None], cos, sin,
            q_norm.astype(F32)[None], k_norm.astype(F32)[None], hid,
            w_q, w_k, w_v, w_o, w_gate, w_up, w_down, k_heads, v_heads)
        k_out, v_out = place(my_pos, k_heads, v_heads, k_rx, v_rx, kn, vn)
        return (out.reshape(STEPS, ROWS, D), k_out.reshape(ROWS, T, 8, HD), v_out.reshape(ROWS, T, 8, HD))

    return jax.shard_map(local_run, mesh=mesh, in_specs=(P('dp'), row_spec, cache_in, cache_in) + (P(),) * 11, out_specs=(row_spec, cache_out, cache_out), check_vma=False)
```

```python
import jax
import numpy as np
import jax.numpy as jnp
from jax import lax
from jax.experimental import pallas as pl
from jax.experimental.pallas import tpu as pltpu
from jax.sharding import PartitionSpec as P

EPS = 1e-6
THETA = 1000000.0
F32 = jnp.float32
BF16 = jnp.bfloat16
MESH = pl.DeviceIdType.MESH

STEPS = 4
ROWS = 32
TOK = STEPS * ROWS
GROUP = 128
D = 5120
HD = 128
QH = 16
FF = 25600
T = 256
SEQ = 4
PER = ROWS // SEQ
NS = 2
NR = 4
NC = 5
N_O = 32
N_C = FF // 256
N_D = FF // 256
LATE = 2
PARTS = ((0, 2), (2, 1), (3, 1), (4, 1), (5, ROWS - LATE - 5))


def partners(me):
    c1 = me + 1 - 2 * lax.rem(me, 2)
    c2 = lax.rem(me + 2, 4)
    c3 = 3 - me
    return c1, c2, c3


def greet(devices):
    barrier = pltpu.get_barrier_semaphore()
    for dev in devices:
        pl.semaphore_signal(barrier, inc=1, device_id={"x": dev}, device_id_type=MESH)
    pl.semaphore_wait(barrier, len(devices))


def remote(src, dst, ssem, rsem, dev):
    return pltpu.make_async_remote_copy(
        src_ref=src, dst_ref=dst, send_sem=ssem, recv_sem=rsem,
        device_id={"x": dev}, device_id_type=MESH)


def rope_table():
    half = np.power(np.float32(THETA), -np.arange(HD // 2, dtype=np.float32) * np.float32(2.0 / HD))
    angles = (np.arange(T, dtype=np.float32)[:, None] * half.astype(np.float32)).astype(np.float64)
    cos, sin = np.cos(angles), np.sin(angles)
    return np.concatenate([cos, cos, -sin, sin], axis=1).astype(np.float32)


def layer_kernel(pos, gains, rope, hid, wq, wk, wv, wo, wg, wu, wd, kc, vc, kc2, vc2,
                 out, kn_out, vn_out, k_rx, v_rx, late2, late3,
                 ws, wrow, hall, hn, cos, sin, tscr, kscr, vscr, q, kn, vn, kbuf, vbuf, o_rx, acc,
                 wsem, osem, s1, r1, s2, r2, sf, rf, kvsem, so, ro, lsem,
                 rsem, csem, ks, kr, vs, vr, ns, nr):
    me = lax.axis_index("x")
    c1, c2, c3 = partners(me)
    order = (c2, c3, c1, me)

    gain = gains.at[:, pl.ds(0, D)]
    gain2 = gains.at[:, pl.ds(D, D)]
    qg = gains.at[:, pl.ds(2 * D, HD)]
    kg = gains.at[:, pl.ds(2 * D + HD, HD)]

    def bulk(part):
        first, count = PARTS[part]
        copies = []
        for k, dev in ((1, c2), (2, c3)):
            rows = pl.ds(dev * ROWS + first, count)
            for src, dst, ss, rs in ((kc, k_rx, ks, kr), (vc, v_rx, vs, vr)):
                copies.append(remote(src.at[rows], dst.at[k, pl.ds(first, count)],
                                     ss.at[part, k - 1], rs.at[part, k - 1], dev))
        return copies

    def near_bulk():
        rows = pl.ds(c1 * ROWS, ROWS)
        return (remote(kc.at[rows], k_rx.at[0], ns.at[0], nr.at[0], c1),
                remote(vc.at[rows], v_rx.at[0], ns.at[1], nr.at[1], c1))

    def start_bulk(part):
        for cp in bulk(part):
            cp.start()

    def row_o(i):
        slot = lax.rem(i, NR)
        return pltpu.make_async_copy(wo.at[pl.ds(i * 256, 256)], wrow.at[slot], rsem.at[slot])

    def row_d(i):
        slot = lax.rem(i + N_O, NR)
        return pltpu.make_async_copy(wd.at[pl.ds(i * 256, 256)], wrow.at[slot], rsem.at[slot])

    def col(i):
        slot = lax.rem(i, NC)
        at = pl.ds(pl.multiple_of(i * 256, 256), 256)
        return (pltpu.make_async_copy(wg.at[:, at], ws.at[2 * slot], csem.at[slot, 0]),
                pltpu.make_async_copy(wu.at[:, at], ws.at[2 * slot + 1], csem.at[slot, 1]))

    def owner(step):
        which = step // PER
        return jnp.where(which == 0, c2, jnp.where(which == 1, c3, jnp.where(which == 2, c1, me)))

    def base_of(step):
        return owner(step) * ROWS + lax.rem(step, PER) * SEQ

    def kv_loads(step):
        slot = lax.rem(step, NS)
        rows = pl.ds(base_of(step), SEQ)
        return (pltpu.make_async_copy(kc2.at[rows], kbuf.at[slot], kvsem.at[slot, 0]),
                pltpu.make_async_copy(vc2.at[rows], vbuf.at[slot], kvsem.at[slot, 1]))

    wcopies = []
    for c in range(10):
        if c < 8:
            src = wq.at[:, pl.ds(pl.multiple_of(me * 2048 + c * 256, 256), 256)]
        else:
            src = (wk if c == 8 else wv).at[:, pl.ds(pl.multiple_of(me * 256, 256), 256)]
        wcopies.append(pltpu.make_async_copy(src, ws.at[c], wsem.at[c]))

    greet((c1, c2, c3))
    cross = []
    fwd = []
    for s in range(STEPS):
        row = 256 + (s // 2) * 128 + (s % 2) * 32
        cross.append(remote(hid.at[pl.ds(s * 32, 32)], hall.at[pl.ds(row, 32)], s2.at[s], r2.at[s], c2))
        fwd.append(remote(hall.at[pl.ds(row, 32)], hall.at[pl.ds(row + 64, 32)], sf.at[s], rf.at[s], c1))
    for cp in cross:
        cp.start()
    near = remote(hid, hall.at[pl.ds(128, 128)], s1, r1, c1)
    near.start()
    own = pltpu.make_async_copy(hid, hall.at[pl.ds(0, 128)], osem)
    own.start()
    for cp in wcopies:
        cp.start()
    start_bulk(0)
    for step in range(NS):
        for cp in kv_loads(step):
            cp.start()
    for i in range(NR):
        row_o(i).start()

    def rope_step(t, carry):
        for s in range(STEPS):
            both = rope[pl.ds(pos[t] + s, 1), :]
            at = pl.ds((t // ROWS) * TOK + s * ROWS + lax.rem(t, ROWS), 1)
            cos[at, :] = both[:, :HD]
            sin[at, :] = both[:, HD:]
        return carry

    lax.fori_loop(0, GROUP, rope_step, 0)

    def table(ref, groups):
        return jnp.concatenate([ref[pl.ds(j * TOK + s * ROWS, ROWS), :] for j, s in groups], axis=0)

    def norm_rows(src, first):
        def norm_step(r, carry):
            val = src[pl.ds(first + r * 16, 16), :].astype(F32)
            inv = lax.rsqrt(jnp.mean(val * val, axis=-1, keepdims=True) + EPS)
            hn[pl.ds(r * 16, 16), :] = (val * inv * gain[...]).astype(BF16)
            return carry

        lax.fori_loop(0, TOK // 16, norm_step, 0)

    def head_fn(groups):
        cos_b = table(cos, groups)
        sin_b = table(sin, groups)

        def head(val, head_gain):
            inv = lax.rsqrt(jnp.mean(val * val, axis=-1, keepdims=True) + EPS)
            val = val * inv * head_gain
            return val * cos_b + pltpu.roll(val, 64, 1) * sin_b

        return head

    def project(c):
        return jnp.dot(hn[...], ws[c], preferred_element_type=F32)

    for blk in range(4):
        if blk == 0:
            own.wait()
            groups = [(me, s) for s in range(4)]
        elif blk == 1:
            near.wait_recv()
            groups = [(c1, s) for s in range(4)]
        else:
            lo = (blk - 2) * 2
            for s in (lo, lo + 1):
                cross[s].wait_recv()
                fwd[s].start()
            for s in (lo, lo + 1):
                fwd[s].wait_recv()
            groups = [(c2, lo), (c2, lo + 1), (c3, lo), (c3, lo + 1)]

        norm_rows(hall, blk * 128)
        head = head_fn(groups)

        def q_chunk(c, carry, head=head):
            val = project(c)
            for hh in range(2):
                tscr[pl.ds(2 * c + hh, 128, stride=QH), :] = head(val[:, hh * HD:(hh + 1) * HD], qg[...])
            return carry

        if blk == 0:
            for cp in wcopies:
                cp.wait()
        lax.fori_loop(0, 8, q_chunk, 0)
        k_acc = project(8)
        v_acc = project(9)
        for hh in range(2):
            k_head = head(k_acc[:, hh * HD:(hh + 1) * HD], kg[...])
            v_head = v_acc[:, hh * HD:(hh + 1) * HD]
            for g, (j, s) in enumerate(groups):
                at = pl.ds(j * 256 + s * 2 + hh, 32, stride=8)
                kscr[at, :] = k_head[g * 32:(g + 1) * 32]
                vscr[at, :] = v_head[g * 32:(g + 1) * 32]
        for g, (j, s) in enumerate(groups):
            q[s, pl.ds(j * 32, 32)] = tscr[pl.ds(g * 512, 512), :].reshape(32, QH, HD).astype(BF16)
    kn[...] = kscr[...].reshape(GROUP, 8, HD).astype(BF16)
    vn[...] = vscr[...].reshape(GROUP, 8, HD).astype(BF16)
    for s in range(STEPS):
        cross[s].wait_send()
        fwd[s].wait_send()
    near.wait_send()

    def o_copy(k):
        return remote(hall.at[pl.ds(k * TOK, TOK), pl.ds(0, 2048)],
                      o_rx.at[:, pl.ds(pl.multiple_of(me * 2048, 2048), 2048)], so.at[k], ro.at[k], order[k])

    row = lax.broadcasted_iota(jnp.int32, (64, 2 * T), 0)
    lane = lax.broadcasted_iota(jnp.int32, (64, 2 * T), 1)
    same_head = lax.rem(row // 8, 2) == lax.rem(lane, 2)
    nrow = lax.broadcasted_iota(jnp.int32, (64, 8), 0)
    nlane = lax.broadcasted_iota(jnp.int32, (64, 8), 1)
    new_ok = (lax.rem(nrow // 8, 2) == lax.rem(nlane, 2)) & (nlane // 2 <= nrow // 16)
    scale = HD ** -0.5
    dims = (((1,), (1,)), ((), ()))

    for k in range(4):
        def attend(j, carry, k=k):
            step = k * PER + j
            slot = lax.rem(step, NS)
            base = base_of(step)
            for cp in kv_loads(step):
                cp.wait()
            for i in range(SEQ):
                start = pos[base + i]
                q2 = q[:, base + i].reshape(64, HD)
                s_old = lax.dot_general(q2, kbuf[slot, i], dims, preferred_element_type=F32) * scale
                s_old = jnp.where(same_head & (lane < 2 * start), s_old, -jnp.inf)
                s_new = lax.dot_general(q2, kn[base + i], dims, preferred_element_type=F32) * scale
                s_new = jnp.where(new_ok, s_new, -jnp.inf)
                peak = jnp.maximum(jnp.max(s_old, axis=-1, keepdims=True), jnp.max(s_new, axis=-1, keepdims=True))
                w_old = jnp.exp(s_old - peak)
                w_new = jnp.exp(s_new - peak)
                total = jnp.sum(w_old, axis=-1, keepdims=True) + jnp.sum(w_new, axis=-1, keepdims=True)
                mixed = jnp.dot(w_old.astype(BF16), vbuf[slot, i], preferred_element_type=F32)
                mixed = mixed + jnp.dot(w_new.astype(BF16), vn[base + i], preferred_element_type=F32)
                tscr[pl.ds(j * SEQ + i, 64, stride=ROWS), :] = mixed / total

            @pl.when(step + NS < 4 * PER)
            def _():
                for cp in kv_loads(step + NS):
                    cp.start()

            @pl.when(j == 1)
            def _():
                if k > 0:
                    o_copy(k - 1).start()
                start_bulk(k + 1)
                if k == 3:
                    for cp in near_bulk():
                        cp.start()
            return carry

        if k == 0:
            for i in range(NC):
                for cp in col(i):
                    cp.start()
        lax.fori_loop(0, PER, attend, 0)
        for s in range(STEPS):
            for hg in range(QH):
                val = tscr[pl.ds((s * QH + hg) * ROWS, ROWS), :].astype(BF16)
                if k < 3:
                    hall[k * TOK + s * ROWS:k * TOK + (s + 1) * ROWS, hg * HD:(hg + 1) * HD] = val
                else:
                    o_rx[s * ROWS:(s + 1) * ROWS, pl.ds(pl.multiple_of(me * 2048 + hg * HD, HD), HD)] = val

    acc[...] = jnp.zeros_like(acc)
    for k in (2, 0, 1):
        o_copy(k).wait()

    def accumulate(lhs, slot):
        for n in range(10):
            cols = slice(n * 512, (n + 1) * 512)
            acc[:, cols] = acc[:, cols] + jnp.dot(lhs, wrow[slot, :, cols], preferred_element_type=F32)

    def o_step(i, carry):
        row_o(i).wait()
        accumulate(o_rx[:, pl.ds(pl.multiple_of(i * 256, 256), 256)], lax.rem(i, NR))

        @pl.when(i + NR < N_O)
        def _():
            row_o(i + NR).start()

        @pl.when(i + NR >= N_O)
        def _():
            row_d(i + NR - N_O).start()
        return carry

    lax.fori_loop(0, N_O, o_step, 0)

    def norm2_step(r, carry):
        rows = pl.ds(r * 16, 16)
        res = (hid[rows, :].astype(F32) + acc[rows, :]).astype(BF16)
        out[rows, :] = res
        res = res.astype(F32)
        inv = lax.rsqrt(jnp.mean(res * res, axis=-1, keepdims=True) + EPS)
        hn[rows, :] = (res * inv * gain2[...]).astype(BF16)
        acc[rows, :] = jnp.zeros((16, D), F32)
        return carry

    lax.fori_loop(0, TOK // 16, norm2_step, 0)

    def act_at(i):
        return pl.ds((i // 20) * 128, 128), pl.ds(pl.multiple_of(lax.rem(i, 20) * 256, 256), 256)

    def col_step(i, carry):
        slot = lax.rem(i, NC)
        for cp in col(i):
            cp.wait()
        gate = jnp.dot(hn[...], ws[2 * slot], preferred_element_type=F32)
        up = jnp.dot(hn[...], ws[2 * slot + 1], preferred_element_type=F32)
        rows, cols = act_at(i)
        hall[rows, cols] = (gate * jax.nn.sigmoid(gate) * up).astype(BF16)

        @pl.when(i + NC < N_C)
        def _():
            for cp in col(i + NC):
                cp.start()
        return carry

    lax.fori_loop(0, N_C, col_step, 0)

    def d_step(i, carry):
        row_d(i).wait()
        rows, cols = act_at(i)
        accumulate(hall[rows, cols], lax.rem(i + N_O, NR))

        @pl.when(i + NR < N_D)
        def _():
            row_d(i + NR).start()
        return carry

    new_w = [pltpu.make_async_copy((wk if c < 4 else wv).at[:, pl.ds((c % 4) * 256, 256)], ws.at[c], wsem.at[c])
             for c in range(8)]
    for cp in new_w:
        cp.start()

    late = []
    for a, (src, buf, d2, d3) in enumerate(((kc2, kbuf, late2.at[0], late3.at[0]), (vc2, vbuf, late2.at[1], late3.at[1]))):
        for b, (dev, dst) in enumerate(((c2, d2), (c3, d3))):
            mid = buf.at[0, pl.ds(b * LATE, LATE)]
            late.append((pltpu.make_async_copy(src.at[pl.ds(dev * ROWS + ROWS - LATE, LATE)], mid, lsem.at[a, b]),
                         pltpu.make_async_copy(mid, dst, lsem.at[a, b])))
    for cp, _ in late:
        cp.start()

    lax.fori_loop(0, N_D, d_step, 0)

    for into, outof in late:
        into.wait()
        outof.start()
    groups = [(me, s) for s in range(STEPS)]
    norm_rows(hid, 0)
    head = head_fn(groups)
    for c in range(8):
        new_w[c].wait()
        val = project(c)
        for hh in range(2):
            one = val[:, hh * HD:(hh + 1) * HD]
            if c < 4:
                one = head(one, kg[...])
            for s in range(STEPS):
                at = pl.ds(s * 8 + (c % 4) * 2 + hh, ROWS, stride=STEPS * 8)
                (kscr if c < 4 else vscr)[at, :] = one[s * ROWS:(s + 1) * ROWS]
    kn_out[...] = kscr[...].reshape(ROWS, STEPS * 8, HD).astype(BF16)
    vn_out[...] = vscr[...].reshape(ROWS, STEPS * 8, HD).astype(BF16)

    def out_step(r, carry):
        rows = pl.ds(r * 16, 16)
        out[rows, :] = (out[rows, :].astype(F32) + acc[rows, :]).astype(BF16)
        return carry

    lax.fori_loop(0, TOK // 16, out_step, 0)
    for _, outof in late:
        outof.wait()
    for cp in near_bulk():
        cp.wait()
    for part in range(len(PARTS)):
        for cp in bulk(part):
            cp.wait()


def layer(pos, gains, rope, hid, wq, wk, wv, wo, wg, wu, wd, kc, vc):
    vmem = pl.BlockSpec(memory_space=pltpu.VMEM)
    hbm = pl.BlockSpec(memory_space=pl.ANY)
    dma = pltpu.SemaphoreType.DMA
    new = jax.ShapeDtypeStruct((ROWS, STEPS * 8, HD), BF16)
    late = jax.ShapeDtypeStruct((2, LATE, 2 * T, HD), BF16)
    rx = jax.ShapeDtypeStruct((3, ROWS, T, 2, HD), BF16)
    n_parts = len(PARTS)
    return pl.pallas_call(
        layer_kernel,
        out_shape=(jax.ShapeDtypeStruct((TOK, D), BF16), new, new, rx, rx, late, late),
        in_specs=[pl.BlockSpec(memory_space=pltpu.SMEM)] + [vmem] * 3 + [hbm] * 11,
        out_specs=(vmem,) * 3 + (hbm,) * 4,
        scratch_shapes=[
            pltpu.VMEM((10, D, 256), BF16),
            pltpu.VMEM((NR, 256, D), BF16),
            pltpu.VMEM((640, D), BF16),
            pltpu.VMEM((TOK, D), BF16),
            pltpu.VMEM((512, HD), F32), pltpu.VMEM((512, HD), F32),
            pltpu.VMEM((2048, HD), F32),
            pltpu.VMEM((GROUP * 8, HD), F32), pltpu.VMEM((GROUP * 8, HD), F32),
            pltpu.VMEM((STEPS, GROUP, QH, HD), BF16),
            pltpu.VMEM((GROUP, 8, HD), BF16), pltpu.VMEM((GROUP, 8, HD), BF16),
            pltpu.VMEM((NS, SEQ, 2 * T, HD), BF16), pltpu.VMEM((NS, SEQ, 2 * T, HD), BF16),
            pltpu.VMEM((TOK, 8192), BF16),
            pltpu.VMEM((TOK, D), F32),
            dma((10,)), dma, dma, dma, dma((4,)), dma((4,)), dma((4,)), dma((4,)), dma((NS, 2)),
            dma((3,)), dma((3,)), dma((2, 2)),
            dma((NR,)), dma((NC, 2)),
            dma((n_parts, 2)), dma((n_parts, 2)), dma((n_parts, 2)), dma((n_parts, 2)), dma((2,)), dma((2,))],
        compiler_params=pltpu.CompilerParams(collective_id=0, has_side_effects=True, vmem_limit_bytes=67043328),
        cost_estimate=pl.CostEstimate(flops=2 * TOK * D * (18432 + 3 * FF), bytes_accessed=1000 << 20, transcendentals=0),
        name="layer",
    )(pos, gains, rope, hid, wq, wk, wv, wo, wg, wu, wd, kc, vc,
      kc.reshape(GROUP, 2 * T, HD), vc.reshape(GROUP, 2 * T, HD))


AR = 8


def place_body(first, count, pos, arrays, isem, osem):
    me = lax.axis_index("x")

    def loads(i):
        slot = i % AR
        copies = []
        for a, (blocks, _, _, buf) in enumerate(arrays):
            for k, (src, dev) in enumerate(blocks(first + i)):
                copies.append(pltpu.make_async_copy(src, buf.at[slot, :, dev], isem.at[slot, a, k]))
        return copies

    def stores(i):
        slot = i % AR
        return [pltpu.make_async_copy(buf.at[slot], out.at[first + i], osem.at[slot, a])
                for a, (_, _, out, buf) in enumerate(arrays)]

    incoming = {}
    outgoing = {}
    for i in range(min(count, AR - 2)):
        incoming[i] = loads(i)
        for cp in incoming[i]:
            cp.start()
    for i in range(count):
        for cp in incoming[i]:
            cp.wait()
        start = pos[me * ROWS + first + i]
        for _, new, _, buf in arrays:
            for s in range(STEPS):
                buf[i % AR, start + s] = new[first + i, s]
        outgoing[i] = stores(i)
        for cp in outgoing[i]:
            cp.start()
        if i >= 2:
            for cp in outgoing[i - 2]:
                cp.wait()
        nxt = i + AR - 2
        if nxt < count:
            incoming[nxt] = loads(nxt)
            for cp in incoming[nxt]:
                cp.start()
    for i in range(max(count - 2, 0), count):
        for cp in outgoing[i]:
            cp.wait()


def place_kernel(pos, kc, vc, k_rx, v_rx, kn, vn, k_out, v_out, kbuf, vbuf, isem, osem):
    me = lax.axis_index("x")
    c1, c2, c3 = partners(me)

    def blocks(own, rx):
        return lambda i: ((rx.at[0, i], c1), (rx.at[1, i], c2), (rx.at[2, i], c3), (own.at[me * ROWS + i], me))

    place_body(0, ROWS - LATE, pos, ((blocks(kc, k_rx), kn, k_out, kbuf), (blocks(vc, v_rx), vn, v_out, vbuf)), isem, osem)


def late_kernel(pos, kc, vc, k_rx, v_rx, got2, got3, kn, vn, k_in, v_in, k_out, v_out, kbuf, vbuf, isem, osem):
    me = lax.axis_index("x")
    c1, c2, c3 = partners(me)

    def blocks(own, rx, a):
        return lambda i: ((rx.at[0, i], c1), (got2.at[a, i - ROWS + LATE], c2), (got3.at[a, i - ROWS + LATE], c3),
                          (own.at[me * ROWS + i], me))

    place_body(ROWS - LATE, LATE, pos, ((blocks(kc, k_rx, 0), kn, k_out, kbuf), (blocks(vc, v_rx, 1), vn, v_out, vbuf)), isem, osem)


def place(kernel, name, pos, caches, news, outs):
    hbm = pl.BlockSpec(memory_space=pl.ANY)
    vmem = pl.BlockSpec(memory_space=pltpu.VMEM)
    out = jax.ShapeDtypeStruct((ROWS, T, 4, 2, HD), BF16)
    buf = pltpu.VMEM((AR, T, 4, 2, HD), BF16)
    dma = pltpu.SemaphoreType.DMA
    n_in = 1 + len(caches) + len(news)
    return pl.pallas_call(
        kernel,
        out_shape=(out, out),
        in_specs=[pl.BlockSpec(memory_space=pltpu.SMEM)] + [hbm] * len(caches) + [vmem] * len(news) + [hbm] * len(outs),
        out_specs=(hbm, hbm),
        input_output_aliases={n_in + a: a for a in range(len(outs))},
        scratch_shapes=[buf, buf, dma((AR, 2, 4)), dma((AR, 2))],
        compiler_params=pltpu.CompilerParams(vmem_limit_bytes=60 << 20),
        cost_estimate=pl.CostEstimate(flops=1 << (20 if outs else 34), bytes_accessed=68 << 20, transcendentals=0),
        name=name,
    )(pos, *caches, *news, *outs)


def solution(mesh):
    row_spec = P(None, ('dp', 'x'), None)
    cache_in = P('dp', None, 'x', None)
    cache_out = P(('dp', 'x'), None, None, None)

    def local_run(start_pos, hidden_in, k_heads, v_heads, attn_norm, w_q, w_k, w_v, q_norm, k_norm, w_o, mlp_norm, w_gate, w_up, w_down):
        hid = hidden_in.reshape(TOK, D)
        gains = jnp.concatenate([attn_norm, mlp_norm, q_norm, k_norm]).astype(F32)[None]
        out, kn, vn, k_rx, v_rx, late2, late3 = layer(
            start_pos, gains, jnp.asarray(rope_table()), hid, w_q, w_k, w_v, w_o, w_gate, w_up, w_down, k_heads, v_heads)
        kn = kn.reshape(ROWS, STEPS, 4, 2, HD)
        vn = vn.reshape(ROWS, STEPS, 4, 2, HD)
        got2 = lax.ppermute(late2, 'x', [(i, i ^ 2) for i in range(4)]).reshape(2, LATE, T, 2, HD)
        got3 = lax.ppermute(late3, 'x', [(i, i ^ 3) for i in range(4)]).reshape(2, LATE, T, 2, HD)
        caches = (k_heads, v_heads, k_rx, v_rx)
        outs = place(place_kernel, "place", start_pos, caches, (kn, vn), ())
        k_out, v_out = place(late_kernel, "place_late", start_pos, caches + (got2, got3), (kn, vn), outs)
        return (out.reshape(STEPS, ROWS, D), k_out.reshape(ROWS, T, 8, HD), v_out.reshape(ROWS, T, 8, HD))

    return jax.shard_map(local_run, mesh=mesh, in_specs=(P('dp'), row_spec, cache_in, cache_in) + (P(),) * 11, out_specs=(row_spec, cache_out, cache_out), check_vma=False)
```

```python
import jax
import numpy as np
import jax.numpy as jnp
from jax import lax
from jax.experimental import pallas as pl
from jax.experimental.pallas import tpu as pltpu
from jax.sharding import PartitionSpec as P

EPS = 1e-6
THETA = 1000000.0
F32 = jnp.float32
BF16 = jnp.bfloat16
MESH = pl.DeviceIdType.MESH

STEPS = 4
ROWS = 32
TOK = STEPS * ROWS
GROUP = 128
D = 5120
HD = 128
QH = 16
FF = 25600
T = 256
SEQ = 4
PER = ROWS // SEQ
NS = 2
NR = 4
NC = 5
N_O = 32
N_C = FF // 256
N_D = FF // 256
LATE = 2
PARTS = ((0, 3), (3, 1), (4, 1), (5, 1), (6, ROWS - LATE - 6))


def partners(me):
    c1 = me + 1 - 2 * lax.rem(me, 2)
    c2 = lax.rem(me + 2, 4)
    c3 = 3 - me
    return c1, c2, c3


def greet(devices):
    barrier = pltpu.get_barrier_semaphore()
    for dev in devices:
        pl.semaphore_signal(barrier, inc=1, device_id={"x": dev}, device_id_type=MESH)
    pl.semaphore_wait(barrier, len(devices))


def remote(src, dst, ssem, rsem, dev):
    return pltpu.make_async_remote_copy(
        src_ref=src, dst_ref=dst, send_sem=ssem, recv_sem=rsem,
        device_id={"x": dev}, device_id_type=MESH)


def rope_table():
    half = np.power(np.float32(THETA), -np.arange(HD // 2, dtype=np.float32) * np.float32(2.0 / HD))
    angles = (np.arange(T, dtype=np.float32)[:, None] * half.astype(np.float32)).astype(np.float64)
    cos, sin = np.cos(angles), np.sin(angles)
    return np.concatenate([cos, cos, -sin, sin], axis=1).astype(np.float32)


def layer_kernel(pos, g1, g2, gq, gk, rope_in, hid_in, wq, wk, wv, wo, wg, wu, wd, kc, vc, kc2, vc2,
                 out, kn_out, vn_out, k_rx, v_rx, late2, late3,
                 ws, wrow, hall, hn, hid, rope, gbuf, gqk, gain, gain2, cos, sin, tscr, kscr, vscr, q, kn, vn, kbuf, vbuf, o_rx, acc,
                 wsem, osem, s1, r1, s2, r2, sf, rf, kvsem, so, ro, lsem,
                 rsem, csem, ks, kr, vs, vr, ns, nr, psem):
    me = lax.axis_index("x")
    c1, c2, c3 = partners(me)
    order = (c2, c3, c1, me)

    def bulk(part):
        first, count = PARTS[part]
        copies = []
        for k, dev in ((1, c2), (2, c3)):
            rows = pl.ds(dev * ROWS + first, count)
            for src, dst, ss, rs in ((kc, k_rx, ks, kr), (vc, v_rx, vs, vr)):
                copies.append(remote(src.at[rows], dst.at[k, pl.ds(first, count)],
                                     ss.at[part, k - 1], rs.at[part, k - 1], dev))
        return copies

    def near_bulk():
        rows = pl.ds(c1 * ROWS, ROWS)
        return (remote(kc.at[rows], k_rx.at[0], ns.at[0], nr.at[0], c1),
                remote(vc.at[rows], v_rx.at[0], ns.at[1], nr.at[1], c1))

    def start_bulk(part):
        for cp in bulk(part):
            cp.start()

    def row_o(i):
        slot = lax.rem(i, NR)
        return pltpu.make_async_copy(wo.at[pl.ds(i * 256, 256)], wrow.at[slot], rsem.at[slot])

    def row_d(i):
        slot = lax.rem(i + N_O, NR)
        return pltpu.make_async_copy(wd.at[pl.ds(i * 256, 256)], wrow.at[slot], rsem.at[slot])

    def col(i):
        slot = lax.rem(i, NC)
        at = pl.ds(pl.multiple_of(i * 256, 256), 256)
        return (pltpu.make_async_copy(wg.at[:, at], ws.at[2 * slot], csem.at[slot, 0]),
                pltpu.make_async_copy(wu.at[:, at], ws.at[2 * slot + 1], csem.at[slot, 1]))

    def owner(step):
        which = step // PER
        return jnp.where(which == 0, c2, jnp.where(which == 1, c3, jnp.where(which == 2, c1, me)))

    def base_of(step):
        return owner(step) * ROWS + lax.rem(step, PER) * SEQ

    def kv_loads(step):
        slot = lax.rem(step, NS)
        rows = pl.ds(base_of(step), SEQ)
        return (pltpu.make_async_copy(kc2.at[rows], kbuf.at[slot], kvsem.at[slot, 0]),
                pltpu.make_async_copy(vc2.at[rows], vbuf.at[slot], kvsem.at[slot, 1]))

    wcopies = []
    for c in range(10):
        if c < 8:
            src = wq.at[:, pl.ds(pl.multiple_of(me * 2048 + c * 256, 256), 256)]
        else:
            src = (wk if c == 8 else wv).at[:, pl.ds(pl.multiple_of(me * 256, 256), 256)]
        wcopies.append(pltpu.make_async_copy(src, ws.at[c], wsem.at[c]))

    greet((c1, c2, c3))
    cross = []
    fwd = []
    for s in range(STEPS):
        row = 256 + (s // 2) * 128 + (s % 2) * 32
        cross.append(remote(hid_in.at[pl.ds(s * 32, 32)], hall.at[pl.ds(row, 32)], s2.at[s], r2.at[s], c2))
        fwd.append(remote(hall.at[pl.ds(row, 32)], hall.at[pl.ds(row + 64, 32)], sf.at[s], rf.at[s], c1))
    for cp in cross:
        cp.start()
    near = remote(hid_in, hall.at[pl.ds(128, 128)], s1, r1, c1)
    near.start()
    own = pltpu.make_async_copy(hid_in, hid, osem)
    own.start()
    small = [pltpu.make_async_copy(src, dst, psem.at[n]) for n, (src, dst) in enumerate((
        (g1, gbuf.at[0]), (g2, gbuf.at[1]), (gq, gqk.at[0]), (gk, gqk.at[1]), (rope_in, rope)))]
    for cp in small:
        cp.start()
    for cp in wcopies:
        cp.start()
    start_bulk(0)
    for step in range(NS):
        for cp in kv_loads(step):
            cp.start()
    for i in range(NR):
        row_o(i).start()

    for cp in small:
        cp.wait()
    for src, dst in ((0, gain), (1, gain2)):
        val = gbuf[src].astype(F32)
        for c in range(D // HD):
            dst[:, c * HD:(c + 1) * HD] = val[c:c + 1, :]
    qg = gqk[0].astype(F32)
    kg = gqk[1].astype(F32)

    def rope_step(t, carry):
        for s in range(STEPS):
            both = rope[pl.ds(pos[t] + s, 1), :]
            at = pl.ds((t // ROWS) * TOK + s * ROWS + lax.rem(t, ROWS), 1)
            cos[at, :] = both[:, :HD]
            sin[at, :] = both[:, HD:]
        return carry

    lax.fori_loop(0, GROUP, rope_step, 0)

    def table(ref, groups):
        return jnp.concatenate([ref[pl.ds(j * TOK + s * ROWS, ROWS), :] for j, s in groups], axis=0)

    def norm_rows(src, first):
        def norm_step(r, carry):
            val = src[pl.ds(first + r * 16, 16), :].astype(F32)
            inv = lax.rsqrt(jnp.mean(val * val, axis=-1, keepdims=True) + EPS)
            hn[pl.ds(r * 16, 16), :] = (val * inv * gain[...]).astype(BF16)
            return carry

        lax.fori_loop(0, TOK // 16, norm_step, 0)

    def head_fn(groups):
        cos_b = table(cos, groups)
        sin_b = table(sin, groups)

        def head(val, head_gain):
            inv = lax.rsqrt(jnp.mean(val * val, axis=-1, keepdims=True) + EPS)
            val = val * inv * head_gain
            return val * cos_b + pltpu.roll(val, 64, 1) * sin_b

        return head

    def project(c):
        return jnp.dot(hn[...], ws[c], preferred_element_type=F32)

    for blk in range(4):
        if blk == 0:
            own.wait()
            groups = [(me, s) for s in range(4)]
        elif blk == 1:
            near.wait_recv()
            groups = [(c1, s) for s in range(4)]
        else:
            lo = (blk - 2) * 2
            for s in (lo, lo + 1):
                cross[s].wait_recv()
                fwd[s].start()
            for s in (lo, lo + 1):
                fwd[s].wait_recv()
            groups = [(c2, lo), (c2, lo + 1), (c3, lo), (c3, lo + 1)]

        if blk == 0:
            norm_rows(hid, 0)
        else:
            norm_rows(hall, blk * 128)
        head = head_fn(groups)

        def q_chunk(c, carry, head=head):
            val = project(c)
            for hh in range(2):
                tscr[pl.ds(2 * c + hh, 128, stride=QH), :] = head(val[:, hh * HD:(hh + 1) * HD], qg)
            return carry

        if blk == 0:
            for cp in wcopies:
                cp.wait()
        lax.fori_loop(0, 8, q_chunk, 0)
        k_acc = project(8)
        v_acc = project(9)
        for hh in range(2):
            k_head = head(k_acc[:, hh * HD:(hh + 1) * HD], kg)
            v_head = v_acc[:, hh * HD:(hh + 1) * HD]
            for g, (j, s) in enumerate(groups):
                at = pl.ds(j * 256 + s * 2 + hh, 32, stride=8)
                kscr[at, :] = k_head[g * 32:(g + 1) * 32]
                vscr[at, :] = v_head[g * 32:(g + 1) * 32]
        for g, (j, s) in enumerate(groups):
            q[s, pl.ds(j * 32, 32)] = tscr[pl.ds(g * 512, 512), :].reshape(32, QH, HD).astype(BF16)
    kn[...] = kscr[...].reshape(GROUP, 8, HD).astype(BF16)
    vn[...] = vscr[...].reshape(GROUP, 8, HD).astype(BF16)
    for s in range(STEPS):
        cross[s].wait_send()
        fwd[s].wait_send()
    near.wait_send()

    def o_copy(k):
        return remote(hall.at[pl.ds(k * TOK, TOK), pl.ds(0, 2048)],
                      o_rx.at[:, pl.ds(pl.multiple_of(me * 2048, 2048), 2048)], so.at[k], ro.at[k], order[k])

    row = lax.broadcasted_iota(jnp.int32, (64, 2 * T), 0)
    lane = lax.broadcasted_iota(jnp.int32, (64, 2 * T), 1)
    same_head = lax.rem(row // 8, 2) == lax.rem(lane, 2)
    nrow = lax.broadcasted_iota(jnp.int32, (64, 8), 0)
    nlane = lax.broadcasted_iota(jnp.int32, (64, 8), 1)
    new_ok = (lax.rem(nrow // 8, 2) == lax.rem(nlane, 2)) & (nlane // 2 <= nrow // 16)
    scale = HD ** -0.5
    dims = (((1,), (1,)), ((), ()))

    for k in range(4):
        def attend(j, carry, k=k):
            step = k * PER + j
            slot = lax.rem(step, NS)
            base = base_of(step)
            for cp in kv_loads(step):
                cp.wait()
            for i in range(SEQ):
                start = pos[base + i]
                q2 = q[:, base + i].reshape(64, HD)
                s_old = lax.dot_general(q2, kbuf[slot, i], dims, preferred_element_type=F32) * scale
                s_old = jnp.where(same_head & (lane < 2 * start), s_old, -jnp.inf)
                s_new = lax.dot_general(q2, kn[base + i], dims, preferred_element_type=F32) * scale
                s_new = jnp.where(new_ok, s_new, -jnp.inf)
                peak = jnp.maximum(jnp.max(s_old, axis=-1, keepdims=True), jnp.max(s_new, axis=-1, keepdims=True))
                w_old = jnp.exp(s_old - peak)
                w_new = jnp.exp(s_new - peak)
                total = jnp.sum(w_old, axis=-1, keepdims=True) + jnp.sum(w_new, axis=-1, keepdims=True)
                mixed = jnp.dot(w_old.astype(BF16), vbuf[slot, i], preferred_element_type=F32)
                mixed = mixed + jnp.dot(w_new.astype(BF16), vn[base + i], preferred_element_type=F32)
                tscr[pl.ds(j * SEQ + i, 64, stride=ROWS), :] = mixed / total

            @pl.when(step + NS < 4 * PER)
            def _():
                for cp in kv_loads(step + NS):
                    cp.start()

            @pl.when(j == 1)
            def _():
                if k > 0:
                    o_copy(k - 1).start()
                start_bulk(k + 1)
                if k == 3:
                    for cp in near_bulk():
                        cp.start()
            return carry

        if k == 0:
            for i in range(NC):
                for cp in col(i):
                    cp.start()
        lax.fori_loop(0, PER, attend, 0)
        for s in range(STEPS):
            for hg in range(QH):
                val = tscr[pl.ds((s * QH + hg) * ROWS, ROWS), :].astype(BF16)
                if k < 3:
                    hall[k * TOK + s * ROWS:k * TOK + (s + 1) * ROWS, hg * HD:(hg + 1) * HD] = val
                else:
                    o_rx[s * ROWS:(s + 1) * ROWS, pl.ds(pl.multiple_of(me * 2048 + hg * HD, HD), HD)] = val

    acc[...] = jnp.zeros_like(acc)
    for k in (2, 0, 1):
        o_copy(k).wait()

    def accumulate(lhs, slot):
        for n in range(10):
            cols = slice(n * 512, (n + 1) * 512)
            acc[:, cols] = acc[:, cols] + jnp.dot(lhs, wrow[slot, :, cols], preferred_element_type=F32)

    def o_step(i, carry):
        row_o(i).wait()
        accumulate(o_rx[:, pl.ds(pl.multiple_of(i * 256, 256), 256)], lax.rem(i, NR))

        @pl.when(i + NR < N_O)
        def _():
            row_o(i + NR).start()

        @pl.when(i + NR >= N_O)
        def _():
            row_d(i + NR - N_O).start()
        return carry

    lax.fori_loop(0, N_O, o_step, 0)

    def norm2_step(r, carry):
        rows = pl.ds(r * 16, 16)
        res = (hid[rows, :].astype(F32) + acc[rows, :]).astype(BF16)
        out[rows, :] = res
        res = res.astype(F32)
        inv = lax.rsqrt(jnp.mean(res * res, axis=-1, keepdims=True) + EPS)
        hn[rows, :] = (res * inv * gain2[...]).astype(BF16)
        acc[rows, :] = jnp.zeros((16, D), F32)
        return carry

    lax.fori_loop(0, TOK // 16, norm2_step, 0)

    def act_at(i):
        return pl.ds((i // 20) * 128, 128), pl.ds(pl.multiple_of(lax.rem(i, 20) * 256, 256), 256)

    def col_step(i, carry):
        slot = lax.rem(i, NC)
        for cp in col(i):
            cp.wait()
        gate = jnp.dot(hn[...], ws[2 * slot], preferred_element_type=F32)
        up = jnp.dot(hn[...], ws[2 * slot + 1], preferred_element_type=F32)
        rows, cols = act_at(i)
        hall[rows, cols] = (gate * jax.nn.sigmoid(gate) * up).astype(BF16)

        @pl.when(i + NC < N_C)
        def _():
            for cp in col(i + NC):
                cp.start()
        return carry

    lax.fori_loop(0, N_C, col_step, 0)

    def d_step(i, carry):
        row_d(i).wait()
        rows, cols = act_at(i)
        accumulate(hall[rows, cols], lax.rem(i + N_O, NR))

        @pl.when(i + NR < N_D)
        def _():
            row_d(i + NR).start()
        return carry

    new_w = [pltpu.make_async_copy((wk if c < 4 else wv).at[:, pl.ds((c % 4) * 256, 256)], ws.at[c], wsem.at[c])
             for c in range(8)]
    for cp in new_w:
        cp.start()

    late = []
    for a, (src, buf, d2, d3) in enumerate(((kc2, kbuf, late2.at[0], late3.at[0]), (vc2, vbuf, late2.at[1], late3.at[1]))):
        for b, (dev, dst) in enumerate(((c2, d2), (c3, d3))):
            mid = buf.at[0, pl.ds(b * LATE, LATE)]
            late.append((pltpu.make_async_copy(src.at[pl.ds(dev * ROWS + ROWS - LATE, LATE)], mid, lsem.at[a, b]),
                         pltpu.make_async_copy(mid, dst, lsem.at[a, b])))
    for cp, _ in late:
        cp.start()

    lax.fori_loop(0, N_D, d_step, 0)

    for into, outof in late:
        into.wait()
        outof.start()
    groups = [(me, s) for s in range(STEPS)]
    norm_rows(hid, 0)
    head = head_fn(groups)
    for c in range(8):
        new_w[c].wait()
        val = project(c)
        for hh in range(2):
            one = val[:, hh * HD:(hh + 1) * HD]
            if c < 4:
                one = head(one, kg)
            for s in range(STEPS):
                at = pl.ds(s * 8 + (c % 4) * 2 + hh, ROWS, stride=STEPS * 8)
                (kscr if c < 4 else vscr)[at, :] = one[s * ROWS:(s + 1) * ROWS]
    kn_out[...] = kscr[...].reshape(ROWS, STEPS * 8, HD).astype(BF16)
    vn_out[...] = vscr[...].reshape(ROWS, STEPS * 8, HD).astype(BF16)

    def out_step(r, carry):
        rows = pl.ds(r * 16, 16)
        out[rows, :] = (out[rows, :].astype(F32) + acc[rows, :]).astype(BF16)
        return carry

    lax.fori_loop(0, TOK // 16, out_step, 0)
    for _, outof in late:
        outof.wait()
    for cp in near_bulk():
        cp.wait()
    for part in range(len(PARTS)):
        for cp in bulk(part):
            cp.wait()


def layer(pos, g1, g2, gq, gk, rope, hid, wq, wk, wv, wo, wg, wu, wd, kc, vc):
    vmem = pl.BlockSpec(memory_space=pltpu.VMEM)
    hbm = pl.BlockSpec(memory_space=pl.ANY)
    dma = pltpu.SemaphoreType.DMA
    new = jax.ShapeDtypeStruct((ROWS, STEPS * 8, HD), BF16)
    late = jax.ShapeDtypeStruct((2, LATE, 2 * T, HD), BF16)
    rx = jax.ShapeDtypeStruct((3, ROWS, T, 2, HD), BF16)
    n_parts = len(PARTS)
    return pl.pallas_call(
        layer_kernel,
        out_shape=(jax.ShapeDtypeStruct((TOK, D), BF16), new, new, rx, rx, late, late),
        in_specs=[pl.BlockSpec(memory_space=pltpu.SMEM)] + [hbm] * 17,
        out_specs=(vmem,) * 3 + (hbm,) * 4,
        scratch_shapes=[
            pltpu.VMEM((10, D, 256), BF16),
            pltpu.VMEM((NR, 256, D), BF16),
            pltpu.VMEM((640, D), BF16),
            pltpu.VMEM((TOK, D), BF16),
            pltpu.VMEM((TOK, D), BF16), pltpu.VMEM((T, 2 * HD), F32),
            pltpu.VMEM((2, D // HD, HD), BF16), pltpu.VMEM((2, 1, HD), BF16),
            pltpu.VMEM((1, D), F32), pltpu.VMEM((1, D), F32),
            pltpu.VMEM((512, HD), F32), pltpu.VMEM((512, HD), F32),
            pltpu.VMEM((2048, HD), F32),
            pltpu.VMEM((GROUP * 8, HD), F32), pltpu.VMEM((GROUP * 8, HD), F32),
            pltpu.VMEM((STEPS, GROUP, QH, HD), BF16),
            pltpu.VMEM((GROUP, 8, HD), BF16), pltpu.VMEM((GROUP, 8, HD), BF16),
            pltpu.VMEM((NS, SEQ, 2 * T, HD), BF16), pltpu.VMEM((NS, SEQ, 2 * T, HD), BF16),
            pltpu.VMEM((TOK, 8192), BF16),
            pltpu.VMEM((TOK, D), F32),
            dma((10,)), dma, dma, dma, dma((4,)), dma((4,)), dma((4,)), dma((4,)), dma((NS, 2)),
            dma((3,)), dma((3,)), dma((2, 2)),
            dma((NR,)), dma((NC, 2)),
            dma((n_parts, 2)), dma((n_parts, 2)), dma((n_parts, 2)), dma((n_parts, 2)), dma((2,)), dma((2,)), dma((5,))],
        compiler_params=pltpu.CompilerParams(collective_id=0, has_side_effects=True, vmem_limit_bytes=67043328),
        cost_estimate=pl.CostEstimate(flops=2 * TOK * D * (18432 + 3 * FF), bytes_accessed=1000 << 20, transcendentals=0),
        name="layer",
    )(pos, g1, g2, gq, gk, rope, hid, wq, wk, wv, wo, wg, wu, wd, kc, vc,
      kc.reshape(GROUP, 2 * T, HD), vc.reshape(GROUP, 2 * T, HD))


AR = 8


def place_kernel(pos, kc, vc, k_rx, v_rx, kn, vn, hid, k_out, v_out, hid_out, kbuf, vbuf, isem, osem, hsem):
    me = lax.axis_index("x")
    c1, c2, c3 = partners(me)
    arrays = ((kc, k_rx, kn, k_out, kbuf), (vc, v_rx, vn, v_out, vbuf))
    hid_copy = pltpu.make_async_copy(hid, hid_out, hsem)

    def late(i):
        return i >= ROWS - LATE

    def loads(i):
        slot = i % AR
        copies = []
        for a, (own, rx, _, _, buf) in enumerate(arrays):
            blocks = [(own.at[me * ROWS + i], me), (rx.at[0, i], c1)]
            if not late(i):
                blocks += [(rx.at[1, i], c2), (rx.at[2, i], c3)]
            for k, (src, dev) in enumerate(blocks):
                copies.append(pltpu.make_async_copy(src, buf.at[slot, :, dev], isem.at[slot, a, k]))
        return copies

    def stores(i):
        slot = i % AR
        copies = []
        for a, (_, _, _, out, buf) in enumerate(arrays):
            if late(i):
                for k, dev in enumerate((me, c1)):
                    copies.append(pltpu.make_async_copy(buf.at[slot, :, dev], out.at[i, :, dev], osem.at[slot, a, k]))
            else:
                copies.append(pltpu.make_async_copy(buf.at[slot], out.at[i], osem.at[slot, a, 0]))
        return copies

    incoming = {}
    outgoing = {}
    for i in range(AR - 2):
        incoming[i] = loads(i)
        for cp in incoming[i]:
            cp.start()
    hid_copy.start()
    for i in range(ROWS):
        for cp in incoming[i]:
            cp.wait()
        start = pos[me * ROWS + i]
        for _, _, new, _, buf in arrays:
            for s in range(STEPS):
                buf[i % AR, start + s] = new[i, s]
        outgoing[i] = stores(i)
        for cp in outgoing[i]:
            cp.start()
        if i >= 2:
            for cp in outgoing[i - 2]:
                cp.wait()
        nxt = i + AR - 2
        if nxt < ROWS:
            incoming[nxt] = loads(nxt)
            for cp in incoming[nxt]:
                cp.start()
    for i in (ROWS - 2, ROWS - 1):
        for cp in outgoing[i]:
            cp.wait()
    hid_copy.wait()


def late_kernel(pos, got2, got3, kn, vn, k_in, v_in, k_out, v_out, bsem, nsem):
    me = lax.axis_index("x")
    _, c2, c3 = partners(me)
    blocks = []
    news = []
    for a, (new, out) in enumerate(((kn, k_out), (vn, v_out))):
        for d, (got, dev) in enumerate(((got2, c2), (got3, c3))):
            blocks.append(pltpu.make_async_copy(
                got.at[a], out.at[pl.ds(ROWS - LATE, LATE), :, dev], bsem.at[a, d]))
            for b in range(LATE):
                i = ROWS - LATE + b
                news.append(pltpu.make_async_copy(
                    new.at[i, :, dev], out.at[i, pl.ds(pos[me * ROWS + i], STEPS), dev], nsem.at[a, d, b]))
    for cp in blocks:
        cp.start()
    for cp in blocks:
        cp.wait()
    for cp in news:
        cp.start()
    for cp in news:
        cp.wait()


def place(pos, caches, news, hid):
    hbm = pl.BlockSpec(memory_space=pl.ANY)
    vmem = pl.BlockSpec(memory_space=pltpu.VMEM)
    out = jax.ShapeDtypeStruct((ROWS, T, 4, 2, HD), BF16)
    buf = pltpu.VMEM((AR, T, 4, 2, HD), BF16)
    dma = pltpu.SemaphoreType.DMA
    return pl.pallas_call(
        place_kernel,
        out_shape=(out, out, jax.ShapeDtypeStruct((TOK, D), BF16)),
        in_specs=[pl.BlockSpec(memory_space=pltpu.SMEM)] + [hbm] * 4 + [vmem] * 3,
        out_specs=(hbm, hbm, hbm),
        scratch_shapes=[buf, buf, dma((AR, 2, 4)), dma((AR, 2, 2)), dma],
        compiler_params=pltpu.CompilerParams(vmem_limit_bytes=58 << 20),
        cost_estimate=pl.CostEstimate(flops=1 << 34, bytes_accessed=68 << 20, transcendentals=0),
        name="place",
    )(pos, *caches, *news, hid)


def place_late(pos, gots, news, outs):
    hbm = pl.BlockSpec(memory_space=pl.ANY)
    vmem = pl.BlockSpec(memory_space=pltpu.VMEM)
    out = jax.ShapeDtypeStruct((ROWS, T, 4, 2, HD), BF16)
    dma = pltpu.SemaphoreType.DMA
    return pl.pallas_call(
        late_kernel,
        out_shape=(out, out),
        in_specs=[pl.BlockSpec(memory_space=pltpu.SMEM)] + [vmem] * 4 + [hbm] * 2,
        out_specs=(hbm, hbm),
        input_output_aliases={5: 0, 6: 1},
        scratch_shapes=[dma((2, 2)), dma((2, 2, LATE))],
        compiler_params=pltpu.CompilerParams(vmem_limit_bytes=16 << 20),
        cost_estimate=pl.CostEstimate(flops=1 << 20, bytes_accessed=2 << 20, transcendentals=0),
        name="place_late",
    )(pos, *gots, *news, *outs)


def solution(mesh):
    row_spec = P(None, ('dp', 'x'), None)
    cache_in = P('dp', None, 'x', None)
    cache_out = P(('dp', 'x'), None, None, None)

    def local_run(start_pos, hidden_in, k_heads, v_heads, attn_norm, w_q, w_k, w_v, q_norm, k_norm, w_o, mlp_norm, w_gate, w_up, w_down):
        hid = hidden_in.reshape(TOK, D)
        out, kn, vn, k_rx, v_rx, late2, late3 = layer(
            start_pos, attn_norm.reshape(D // HD, HD), mlp_norm.reshape(D // HD, HD), q_norm[None], k_norm[None],
            jnp.asarray(rope_table()), hid, w_q, w_k, w_v, w_o, w_gate, w_up, w_down, k_heads, v_heads)
        kn = kn.reshape(ROWS, STEPS, 4, 2, HD)
        vn = vn.reshape(ROWS, STEPS, 4, 2, HD)
        got2 = lax.ppermute(late2, 'x', [(i, i ^ 2) for i in range(4)]).reshape(2, LATE, T, 2, HD)
        got3 = lax.ppermute(late3, 'x', [(i, i ^ 3) for i in range(4)]).reshape(2, LATE, T, 2, HD)
        k_out, v_out, out = place(start_pos, (k_heads, v_heads, k_rx, v_rx), (kn, vn), out)
        k_out, v_out = place_late(start_pos, (got2, got3), (kn, vn), (k_out, v_out))
        return (out.reshape(STEPS, ROWS, D), k_out.reshape(ROWS, T, 8, HD), v_out.reshape(ROWS, T, 8, HD))

    return jax.shard_map(local_run, mesh=mesh, in_specs=(P('dp'), row_spec, cache_in, cache_in) + (P(),) * 11, out_specs=(row_spec, cache_out, cache_out), check_vma=False)
```

```python
import jax
import numpy as np
import jax.numpy as jnp
from jax import lax
from jax.experimental import pallas as pl
from jax.experimental.pallas import tpu as pltpu
from jax.sharding import PartitionSpec as P

EPS = 1e-6
THETA = 1000000.0
F32 = jnp.float32
BF16 = jnp.bfloat16
MESH = pl.DeviceIdType.MESH

STEPS = 4
ROWS = 32
TOK = STEPS * ROWS
GROUP = 128
D = 5120
HD = 128
QH = 16
FF = 25600
T = 256
SEQ = 4
PER = ROWS // SEQ
NS = 2
NR = 4
NC = 5
N_O = 32
N_C = FF // 256
N_D = FF // 256
LATE = 2
PARTS = ((0, 3), (3, 1), (4, 1), (5, 1), (6, ROWS - LATE - 6))


def partners(me):
    c1 = me + 1 - 2 * lax.rem(me, 2)
    c2 = lax.rem(me + 2, 4)
    c3 = 3 - me
    return c1, c2, c3


def greet(devices):
    barrier = pltpu.get_barrier_semaphore()
    for dev in devices:
        pl.semaphore_signal(barrier, inc=1, device_id={"x": dev}, device_id_type=MESH)
    pl.semaphore_wait(barrier, len(devices))


def remote(src, dst, ssem, rsem, dev):
    return pltpu.make_async_remote_copy(
        src_ref=src, dst_ref=dst, send_sem=ssem, recv_sem=rsem,
        device_id={"x": dev}, device_id_type=MESH)


def rope_table():
    half = np.power(np.float32(THETA), -np.arange(HD // 2, dtype=np.float32) * np.float32(2.0 / HD))
    angles = (np.arange(T, dtype=np.float32)[:, None] * half.astype(np.float32)).astype(np.float64)
    cos, sin = np.cos(angles), np.sin(angles)
    return np.concatenate([cos, cos, -sin, sin], axis=1).astype(np.float32)


def layer_kernel(pos, g1, g2, gq, gk, rope_in, hid_in, wq, wk, wv, wo, wg, wu, wd, kc, vc, kc2, vc2,
                 out, kn_out, vn_out, k_rx, v_rx, late2, late3,
                 ws, wrow, hall, hn, hid, rope, gbuf, gqk, gain, gain2, cos, sin, tscr, kscr, vscr, q, kn, vn, kbuf, vbuf, o_rx, acc,
                 wsem, osem, s1, r1, s2, r2, sf, rf, kvsem, so, ro, lsem,
                 rsem, csem, ks, kr, vs, vr, ns, nr, psem):
    me = lax.axis_index("x")
    c1, c2, c3 = partners(me)
    order = (c2, c3, c1, me)

    def bulk(part):
        first, count = PARTS[part]
        copies = []
        for k, dev in ((1, c2), (2, c3)):
            rows = pl.ds(dev * ROWS + first, count)
            for src, dst, ss, rs in ((kc, k_rx, ks, kr), (vc, v_rx, vs, vr)):
                copies.append(remote(src.at[rows], dst.at[k, pl.ds(first, count)],
                                     ss.at[part, k - 1], rs.at[part, k - 1], dev))
        return copies

    def near_bulk():
        rows = pl.ds(c1 * ROWS, ROWS)
        return (remote(kc.at[rows], k_rx.at[0], ns.at[0], nr.at[0], c1),
                remote(vc.at[rows], v_rx.at[0], ns.at[1], nr.at[1], c1))

    def start_bulk(part):
        for cp in bulk(part):
            cp.start()

    def row_o(i):
        slot = lax.rem(i, NR)
        return pltpu.make_async_copy(wo.at[pl.ds(i * 256, 256)], wrow.at[slot], rsem.at[slot])

    def row_d(i):
        slot = lax.rem(i + N_O, NR)
        return pltpu.make_async_copy(wd.at[pl.ds(i * 256, 256)], wrow.at[slot], rsem.at[slot])

    def col(i):
        slot = lax.rem(i, NC)
        at = pl.ds(pl.multiple_of(i * 256, 256), 256)
        return (pltpu.make_async_copy(wg.at[:, at], ws.at[2 * slot], csem.at[slot, 0]),
                pltpu.make_async_copy(wu.at[:, at], ws.at[2 * slot + 1], csem.at[slot, 1]))

    def owner(step):
        which = step // PER
        return jnp.where(which == 0, c2, jnp.where(which == 1, c3, jnp.where(which == 2, c1, me)))

    def base_of(step):
        return owner(step) * ROWS + lax.rem(step, PER) * SEQ

    def kv_loads(step):
        slot = lax.rem(step, NS)
        rows = pl.ds(base_of(step), SEQ)
        return (pltpu.make_async_copy(kc2.at[rows], kbuf.at[slot], kvsem.at[slot, 0]),
                pltpu.make_async_copy(vc2.at[rows], vbuf.at[slot], kvsem.at[slot, 1]))

    wcopies = []
    for c in range(10):
        if c < 8:
            src = wq.at[:, pl.ds(pl.multiple_of(me * 2048 + c * 256, 256), 256)]
        else:
            src = (wk if c == 8 else wv).at[:, pl.ds(pl.multiple_of(me * 256, 256), 256)]
        wcopies.append(pltpu.make_async_copy(src, ws.at[c], wsem.at[c]))

    greet((c1, c2, c3))
    cross = []
    fwd = []
    for s in range(STEPS):
        row = 256 + (s // 2) * 128 + (s % 2) * 32
        cross.append(remote(hid_in.at[pl.ds(s * 32, 32)], hall.at[pl.ds(row, 32)], s2.at[s], r2.at[s], c2))
        fwd.append(remote(hall.at[pl.ds(row, 32)], hall.at[pl.ds(row + 64, 32)], sf.at[s], rf.at[s], c1))
    for cp in cross:
        cp.start()
    near = remote(hid_in, hall.at[pl.ds(128, 128)], s1, r1, c1)
    near.start()
    own = pltpu.make_async_copy(hid_in, hid, osem)
    own.start()
    small = [pltpu.make_async_copy(src, dst, psem.at[n]) for n, (src, dst) in enumerate((
        (g1, gbuf.at[0]), (g2, gbuf.at[1]), (gq, gqk.at[0]), (gk, gqk.at[1]), (rope_in, rope)))]
    for cp in small:
        cp.start()
    for cp in wcopies:
        cp.start()
    start_bulk(0)
    for step in range(NS):
        for cp in kv_loads(step):
            cp.start()
    for i in range(NR):
        row_o(i).start()

    for cp in small:
        cp.wait()
    for src, dst in ((0, gain), (1, gain2)):
        val = gbuf[src].astype(F32)
        for c in range(D // HD):
            dst[:, c * HD:(c + 1) * HD] = val[c:c + 1, :]
    qg = gqk[0].astype(F32)
    kg = gqk[1].astype(F32)

    def rope_step(t, carry):
        for s in range(STEPS):
            both = rope[pl.ds(pos[t] + s, 1), :]
            at = pl.ds((t // ROWS) * TOK + s * ROWS + lax.rem(t, ROWS), 1)
            cos[at, :] = both[:, :HD]
            sin[at, :] = both[:, HD:]
        return carry

    lax.fori_loop(0, GROUP, rope_step, 0)

    def table(ref, groups):
        return jnp.concatenate([ref[pl.ds(j * TOK + s * ROWS, ROWS), :] for j, s in groups], axis=0)

    def norm_rows(src, first):
        def norm_step(r, carry):
            val = src[pl.ds(first + r * 16, 16), :].astype(F32)
            inv = lax.rsqrt(jnp.mean(val * val, axis=-1, keepdims=True) + EPS)
            hn[pl.ds(r * 16, 16), :] = (val * inv * gain[...]).astype(BF16)
            return carry

        lax.fori_loop(0, TOK // 16, norm_step, 0)

    def head_fn(groups):
        cos_b = table(cos, groups)
        sin_b = table(sin, groups)

        def head(val, head_gain):
            inv = lax.rsqrt(jnp.mean(val * val, axis=-1, keepdims=True) + EPS)
            val = val * inv * head_gain
            return val * cos_b + pltpu.roll(val, 64, 1) * sin_b

        return head

    def project(c):
        return jnp.dot(hn[...], ws[c], preferred_element_type=F32)

    for blk in range(4):
        if blk == 0:
            own.wait()
            groups = [(me, s) for s in range(4)]
        elif blk == 1:
            near.wait_recv()
            groups = [(c1, s) for s in range(4)]
        else:
            lo = (blk - 2) * 2
            for s in (lo, lo + 1):
                cross[s].wait_recv()
                fwd[s].start()
            for s in (lo, lo + 1):
                fwd[s].wait_recv()
            groups = [(c2, lo), (c2, lo + 1), (c3, lo), (c3, lo + 1)]

        if blk == 0:
            norm_rows(hid, 0)
        else:
            norm_rows(hall, blk * 128)
        head = head_fn(groups)

        def q_chunk(c, carry, head=head):
            val = project(c)
            for hh in range(2):
                tscr[pl.ds(2 * c + hh, 128, stride=QH), :] = head(val[:, hh * HD:(hh + 1) * HD], qg)
            return carry

        if blk == 0:
            for cp in wcopies:
                cp.wait()
        lax.fori_loop(0, 8, q_chunk, 0)
        k_acc = project(8)
        v_acc = project(9)
        for hh in range(2):
            k_head = head(k_acc[:, hh * HD:(hh + 1) * HD], kg)
            v_head = v_acc[:, hh * HD:(hh + 1) * HD]
            for g, (j, s) in enumerate(groups):
                at = pl.ds(j * 256 + s * 2 + hh, 32, stride=8)
                kscr[at, :] = k_head[g * 32:(g + 1) * 32]
                vscr[at, :] = v_head[g * 32:(g + 1) * 32]
        for g, (j, s) in enumerate(groups):
            q[s, pl.ds(j * 32, 32)] = tscr[pl.ds(g * 512, 512), :].reshape(32, QH, HD).astype(BF16)
    kn[...] = kscr[...].reshape(GROUP, 8, HD).astype(BF16)
    vn[...] = vscr[...].reshape(GROUP, 8, HD).astype(BF16)
    for s in range(STEPS):
        cross[s].wait_send()
        fwd[s].wait_send()
    near.wait_send()

    def o_copy(k):
        return remote(hall.at[pl.ds(k * TOK, TOK), pl.ds(0, 2048)],
                      o_rx.at[:, pl.ds(pl.multiple_of(me * 2048, 2048), 2048)], so.at[k], ro.at[k], order[k])

    row = lax.broadcasted_iota(jnp.int32, (64, 2 * T), 0)
    lane = lax.broadcasted_iota(jnp.int32, (64, 2 * T), 1)
    same_head = lax.rem(row // 8, 2) == lax.rem(lane, 2)
    nrow = lax.broadcasted_iota(jnp.int32, (64, 8), 0)
    nlane = lax.broadcasted_iota(jnp.int32, (64, 8), 1)
    new_ok = (lax.rem(nrow // 8, 2) == lax.rem(nlane, 2)) & (nlane // 2 <= nrow // 16)
    scale = HD ** -0.5
    dims = (((1,), (1,)), ((), ()))

    for k in range(4):
        def attend(j, carry, k=k):
            step = k * PER + j
            slot = lax.rem(step, NS)
            base = base_of(step)
            for cp in kv_loads(step):
                cp.wait()
            for i in range(SEQ):
                start = pos[base + i]
                q2 = q[:, base + i].reshape(64, HD)
                s_old = lax.dot_general(q2, kbuf[slot, i], dims, preferred_element_type=F32) * scale
                s_old = jnp.where(same_head & (lane < 2 * start), s_old, -jnp.inf)
                s_new = lax.dot_general(q2, kn[base + i], dims, preferred_element_type=F32) * scale
                s_new = jnp.where(new_ok, s_new, -jnp.inf)
                peak = jnp.maximum(jnp.max(s_old, axis=-1, keepdims=True), jnp.max(s_new, axis=-1, keepdims=True))
                w_old = jnp.exp(s_old - peak)
                w_new = jnp.exp(s_new - peak)
                total = jnp.sum(w_old, axis=-1, keepdims=True) + jnp.sum(w_new, axis=-1, keepdims=True)
                mixed = jnp.dot(w_old.astype(BF16), vbuf[slot, i], preferred_element_type=F32)
                mixed = mixed + jnp.dot(w_new.astype(BF16), vn[base + i], preferred_element_type=F32)
                tscr[pl.ds(j * SEQ + i, 64, stride=ROWS), :] = mixed / total

            @pl.when(step + NS < 4 * PER)
            def _():
                for cp in kv_loads(step + NS):
                    cp.start()

            @pl.when(j == 1)
            def _():
                if k > 0:
                    o_copy(k - 1).start()
                start_bulk(k + 1)
                if k == 3:
                    for cp in near_bulk():
                        cp.start()
            return carry

        if k == 0:
            for i in range(NC):
                for cp in col(i):
                    cp.start()
        lax.fori_loop(0, PER, attend, 0)
        for s in range(STEPS):
            for hg in range(QH):
                val = tscr[pl.ds((s * QH + hg) * ROWS, ROWS), :].astype(BF16)
                if k < 3:
                    hall[k * TOK + s * ROWS:k * TOK + (s + 1) * ROWS, hg * HD:(hg + 1) * HD] = val
                else:
                    o_rx[s * ROWS:(s + 1) * ROWS, pl.ds(pl.multiple_of(me * 2048 + hg * HD, HD), HD)] = val

    acc[...] = jnp.zeros_like(acc)
    for k in (2, 0, 1):
        o_copy(k).wait()

    def accumulate(lhs, slot):
        for n in range(10):
            cols = slice(n * 512, (n + 1) * 512)
            acc[:, cols] = acc[:, cols] + jnp.dot(lhs, wrow[slot, :, cols], preferred_element_type=F32)

    def o_step(i, carry):
        row_o(i).wait()
        accumulate(o_rx[:, pl.ds(pl.multiple_of(i * 256, 256), 256)], lax.rem(i, NR))

        @pl.when(i + NR < N_O)
        def _():
            row_o(i + NR).start()

        @pl.when(i + NR >= N_O)
        def _():
            row_d(i + NR - N_O).start()
        return carry

    lax.fori_loop(0, N_O, o_step, 0)

    def norm2_step(r, carry):
        rows = pl.ds(r * 16, 16)
        res = (hid[rows, :].astype(F32) + acc[rows, :]).astype(BF16)
        out[rows, :] = res
        res = res.astype(F32)
        inv = lax.rsqrt(jnp.mean(res * res, axis=-1, keepdims=True) + EPS)
        hn[rows, :] = (res * inv * gain2[...]).astype(BF16)
        acc[rows, :] = jnp.zeros((16, D), F32)
        return carry

    lax.fori_loop(0, TOK // 16, norm2_step, 0)

    def act_at(i):
        return pl.ds((i // 20) * 128, 128), pl.ds(pl.multiple_of(lax.rem(i, 20) * 256, 256), 256)

    def col_step(i, carry):
        slot = lax.rem(i, NC)
        for cp in col(i):
            cp.wait()
        gate = jnp.dot(hn[...], ws[2 * slot], preferred_element_type=F32)
        up = jnp.dot(hn[...], ws[2 * slot + 1], preferred_element_type=F32)
        rows, cols = act_at(i)
        hall[rows, cols] = (gate * jax.nn.sigmoid(gate) * up).astype(BF16)

        @pl.when(i + NC < N_C)
        def _():
            for cp in col(i + NC):
                cp.start()
        return carry

    lax.fori_loop(0, N_C, col_step, 0)

    def d_step(i, carry):
        row_d(i).wait()
        rows, cols = act_at(i)
        accumulate(hall[rows, cols], lax.rem(i + N_O, NR))

        @pl.when(i + NR < N_D)
        def _():
            row_d(i + NR).start()
        return carry

    new_w = [pltpu.make_async_copy((wk if c < 4 else wv).at[:, pl.ds((c % 4) * 256, 256)], ws.at[c], wsem.at[c])
             for c in range(8)]
    for cp in new_w:
        cp.start()

    late = []
    for a, (src, buf, d2, d3) in enumerate(((kc2, kbuf, late2.at[0], late3.at[0]), (vc2, vbuf, late2.at[1], late3.at[1]))):
        for b, (dev, dst) in enumerate(((c2, d2), (c3, d3))):
            mid = buf.at[0, pl.ds(b * LATE, LATE)]
            late.append((pltpu.make_async_copy(src.at[pl.ds(dev * ROWS + ROWS - LATE, LATE)], mid, lsem.at[a, b]),
                         pltpu.make_async_copy(mid, dst, lsem.at[a, b])))
    for cp, _ in late:
        cp.start()

    lax.fori_loop(0, N_D, d_step, 0)

    for into, outof in late:
        into.wait()
        outof.start()
    groups = [(me, s) for s in range(STEPS)]
    norm_rows(hid, 0)
    head = head_fn(groups)
    for c in range(8):
        new_w[c].wait()
        val = project(c)
        for hh in range(2):
            one = val[:, hh * HD:(hh + 1) * HD]
            if c < 4:
                one = head(one, kg)
            for s in range(STEPS):
                at = pl.ds(s * 8 + (c % 4) * 2 + hh, ROWS, stride=STEPS * 8)
                (kscr if c < 4 else vscr)[at, :] = one[s * ROWS:(s + 1) * ROWS]
    kn_out[...] = kscr[...].reshape(ROWS, STEPS * 8, HD).astype(BF16)
    vn_out[...] = vscr[...].reshape(ROWS, STEPS * 8, HD).astype(BF16)

    def out_step(r, carry):
        rows = pl.ds(r * 16, 16)
        out[rows, :] = (out[rows, :].astype(F32) + acc[rows, :]).astype(BF16)
        return carry

    lax.fori_loop(0, TOK // 16, out_step, 0)
    for _, outof in late:
        outof.wait()
    for cp in near_bulk():
        cp.wait()
    for part in range(len(PARTS)):
        for cp in bulk(part):
            cp.wait()


def layer(pos, g1, g2, gq, gk, rope, hid, wq, wk, wv, wo, wg, wu, wd, kc, vc):
    vmem = pl.BlockSpec(memory_space=pltpu.VMEM)
    hbm = pl.BlockSpec(memory_space=pl.ANY)
    dma = pltpu.SemaphoreType.DMA
    new = jax.ShapeDtypeStruct((ROWS, STEPS * 8, HD), BF16)
    late = jax.ShapeDtypeStruct((2, LATE, 2 * T, HD), BF16)
    rx = jax.ShapeDtypeStruct((3, ROWS, T, 2, HD), BF16)
    n_parts = len(PARTS)
    return pl.pallas_call(
        layer_kernel,
        out_shape=(jax.ShapeDtypeStruct((TOK, D), BF16), new, new, rx, rx, late, late),
        in_specs=[pl.BlockSpec(memory_space=pltpu.SMEM)] + [hbm] * 17,
        out_specs=(vmem,) * 3 + (hbm,) * 4,
        scratch_shapes=[
            pltpu.VMEM((10, D, 256), BF16),
            pltpu.VMEM((NR, 256, D), BF16),
            pltpu.VMEM((640, D), BF16),
            pltpu.VMEM((TOK, D), BF16),
            pltpu.VMEM((TOK, D), BF16), pltpu.VMEM((T, 2 * HD), F32),
            pltpu.VMEM((2, D // HD, HD), BF16), pltpu.VMEM((2, 1, HD), BF16),
            pltpu.VMEM((1, D), F32), pltpu.VMEM((1, D), F32),
            pltpu.VMEM((512, HD), F32), pltpu.VMEM((512, HD), F32),
            pltpu.VMEM((2048, HD), F32),
            pltpu.VMEM((GROUP * 8, HD), F32), pltpu.VMEM((GROUP * 8, HD), F32),
            pltpu.VMEM((STEPS, GROUP, QH, HD), BF16),
            pltpu.VMEM((GROUP, 8, HD), BF16), pltpu.VMEM((GROUP, 8, HD), BF16),
            pltpu.VMEM((NS, SEQ, 2 * T, HD), BF16), pltpu.VMEM((NS, SEQ, 2 * T, HD), BF16),
            pltpu.VMEM((TOK, 8192), BF16),
            pltpu.VMEM((TOK, D), F32),
            dma((10,)), dma, dma, dma, dma((4,)), dma((4,)), dma((4,)), dma((4,)), dma((NS, 2)),
            dma((3,)), dma((3,)), dma((2, 2)),
            dma((NR,)), dma((NC, 2)),
            dma((n_parts, 2)), dma((n_parts, 2)), dma((n_parts, 2)), dma((n_parts, 2)), dma((2,)), dma((2,)), dma((5,))],
        compiler_params=pltpu.CompilerParams(collective_id=0, has_side_effects=True, vmem_limit_bytes=67043328),
        cost_estimate=pl.CostEstimate(flops=2 * TOK * D * (18432 + 3 * FF), bytes_accessed=1000 << 20, transcendentals=0),
        name="layer",
    )(pos, g1, g2, gq, gk, rope, hid, wq, wk, wv, wo, wg, wu, wd, kc, vc,
      kc.reshape(GROUP, 2 * T, HD), vc.reshape(GROUP, 2 * T, HD))


PAIR = 2
AR = 5


def place_kernel(pos, kc, vc, k_rx, v_rx, kn, vn, k_out, v_out, kbuf, vbuf, isem, osem):
    me = lax.axis_index("x")
    c1, c2, c3 = partners(me)
    arrays = ((kc, k_rx, kn, k_out, kbuf), (vc, v_rx, vn, v_out, vbuf))
    def late(i):
        return i >= (ROWS - LATE) // PAIR

    def loads(i):
        slot = i % AR
        copies = []
        for a, (own, rx, _, _, buf) in enumerate(arrays):
            seqs = pl.ds(i * PAIR, PAIR)
            blocks = [(own.at[pl.ds(me * ROWS + i * PAIR, PAIR)], me), (rx.at[0, seqs], c1)]
            if not late(i):
                blocks += [(rx.at[1, seqs], c2), (rx.at[2, seqs], c3)]
            for k, (src, dev) in enumerate(blocks):
                copies.append(pltpu.make_async_copy(src, buf.at[slot, :, :, dev], isem.at[slot, a, k]))
        return copies

    def stores(i):
        slot = i % AR
        copies = []
        for a, (_, _, _, out, buf) in enumerate(arrays):
            if late(i):
                for k, dev in enumerate((me, c1)):
                    copies.append(pltpu.make_async_copy(
                        buf.at[slot, :, :, dev], out.at[pl.ds(i * PAIR, PAIR), :, dev], osem.at[slot, a, k]))
            else:
                copies.append(pltpu.make_async_copy(buf.at[slot], out.at[pl.ds(i * PAIR, PAIR)], osem.at[slot, a, 0]))
        return copies

    incoming = {}
    outgoing = {}
    for i in range(AR - 1):
        incoming[i] = loads(i)
        for cp in incoming[i]:
            cp.start()
    for i in range(ROWS // PAIR):
        for cp in incoming[i]:
            cp.wait()
        for b in range(PAIR):
            start = pos[me * ROWS + i * PAIR + b]
            for _, _, new, _, buf in arrays:
                for s in range(STEPS):
                    buf[i % AR, b, start + s] = new[i * PAIR + b, s]
        outgoing[i] = stores(i)
        for cp in outgoing[i]:
            cp.start()
        if i >= 1:
            for cp in outgoing[i - 1]:
                cp.wait()
        nxt = i + AR - 1
        if nxt < ROWS // PAIR:
            incoming[nxt] = loads(nxt)
            for cp in incoming[nxt]:
                cp.start()
    for cp in outgoing[ROWS // PAIR - 1]:
        cp.wait()


def late_kernel(pos, got2, got3, kn, vn, hid, k_in, v_in, k_out, v_out, hid_out, bsem, nsem, hsem):
    me = lax.axis_index("x")
    _, c2, c3 = partners(me)
    blocks = []
    news = []
    for a, (new, out) in enumerate(((kn, k_out), (vn, v_out))):
        for d, (got, dev) in enumerate(((got2, c2), (got3, c3))):
            blocks.append(pltpu.make_async_copy(
                got.at[a], out.at[pl.ds(ROWS - LATE, LATE), :, dev], bsem.at[a, d]))
            for b in range(LATE):
                i = ROWS - LATE + b
                news.append(pltpu.make_async_copy(
                    new.at[i, :, dev], out.at[i, pl.ds(pos[me * ROWS + i], STEPS), dev], nsem.at[a, d, b]))
    for cp in blocks:
        cp.start()
    hid_copy = pltpu.make_async_copy(hid, hid_out, hsem)
    hid_copy.start()
    for cp in blocks:
        cp.wait()
    for cp in news:
        cp.start()
    for cp in news:
        cp.wait()
    hid_copy.wait()


def place(pos, caches, news):
    hbm = pl.BlockSpec(memory_space=pl.ANY)
    vmem = pl.BlockSpec(memory_space=pltpu.VMEM)
    out = jax.ShapeDtypeStruct((ROWS, T, 4, 2, HD), BF16)
    buf = pltpu.VMEM((AR, PAIR, T, 4, 2, HD), BF16)
    dma = pltpu.SemaphoreType.DMA
    return pl.pallas_call(
        place_kernel,
        out_shape=(out, out),
        in_specs=[pl.BlockSpec(memory_space=pltpu.SMEM)] + [hbm] * 4 + [vmem] * 2,
        out_specs=(hbm, hbm),
        scratch_shapes=[buf, buf, dma((AR, 2, 4)), dma((AR, 2, 2))],
        compiler_params=pltpu.CompilerParams(vmem_limit_bytes=58 << 20),
        cost_estimate=pl.CostEstimate(flops=1 << 34, bytes_accessed=68 << 20, transcendentals=0),
        name="place",
    )(pos, *caches, *news)


def place_late(pos, gots, news, hid, outs):
    hbm = pl.BlockSpec(memory_space=pl.ANY)
    vmem = pl.BlockSpec(memory_space=pltpu.VMEM)
    out = jax.ShapeDtypeStruct((ROWS, T, 4, 2, HD), BF16)
    dma = pltpu.SemaphoreType.DMA
    return pl.pallas_call(
        late_kernel,
        out_shape=(out, out, jax.ShapeDtypeStruct((TOK, D), BF16)),
        in_specs=[pl.BlockSpec(memory_space=pltpu.SMEM)] + [vmem] * 5 + [hbm] * 2,
        out_specs=(hbm, hbm, hbm),
        input_output_aliases={6: 0, 7: 1},
        scratch_shapes=[dma((2, 2)), dma((2, 2, LATE)), dma],
        compiler_params=pltpu.CompilerParams(vmem_limit_bytes=16 << 20),
        cost_estimate=pl.CostEstimate(flops=1 << 20, bytes_accessed=2 << 20, transcendentals=0),
        name="place_late",
    )(pos, *gots, *news, hid, *outs)


def solution(mesh):
    row_spec = P(None, ('dp', 'x'), None)
    cache_in = P('dp', None, 'x', None)
    cache_out = P(('dp', 'x'), None, None, None)

    def local_run(start_pos, hidden_in, k_heads, v_heads, attn_norm, w_q, w_k, w_v, q_norm, k_norm, w_o, mlp_norm, w_gate, w_up, w_down):
        hid = hidden_in.reshape(TOK, D)
        out, kn, vn, k_rx, v_rx, late2, late3 = layer(
            start_pos, attn_norm.reshape(D // HD, HD), mlp_norm.reshape(D // HD, HD), q_norm[None], k_norm[None],
            jnp.asarray(rope_table()), hid, w_q, w_k, w_v, w_o, w_gate, w_up, w_down, k_heads, v_heads)
        kn = kn.reshape(ROWS, STEPS, 4, 2, HD)
        vn = vn.reshape(ROWS, STEPS, 4, 2, HD)
        got2 = lax.ppermute(late2, 'x', [(i, i ^ 2) for i in range(4)]).reshape(2, LATE, T, 2, HD)
        got3 = lax.ppermute(late3, 'x', [(i, i ^ 3) for i in range(4)]).reshape(2, LATE, T, 2, HD)
        caches = place(start_pos, (k_heads, v_heads, k_rx, v_rx), (kn, vn))
        k_out, v_out, out = place_late(start_pos, (got2, got3), (kn, vn), out, caches)
        return (out.reshape(STEPS, ROWS, D), k_out.reshape(ROWS, T, 8, HD), v_out.reshape(ROWS, T, 8, HD))

    return jax.shard_map(local_run, mesh=mesh, in_specs=(P('dp'), row_spec, cache_in, cache_in) + (P(),) * 11, out_specs=(row_spec, cache_out, cache_out), check_vma=False)
```
